32 devices in a mesh: dp: 2 (over x), tp: 4 (over z), sp: 4 (over y, core).
Axes of the slice: x: 2, y: 2, z: 4, core: 2. Of those that a mesh axis runs over, the one named last changes fastest.
Arguments:
- x_in: bfloat16 [128, 2048], P('dp'), parts along dimension 0
- seq_lens: int32 [128], P('dp'), parts along dimension 0
- k_cache: bfloat16 [128, 512, 16, 128], P('dp', 'sp', 'tp'), parts along dimension 0
- v_cache: bfloat16 [128, 512, 16, 128], P('dp', 'sp', 'tp'), parts along dimension 0
- ln1_gain: float32 [2048], replicated
- w_qkv: bfloat16 [2048, 3, 16, 128], P(None, None, 'tp')
- w_out: bfloat16 [16, 128, 2048], P('tp')
- ln2_gain: float32 [2048], replicated
- w_up: bfloat16 [2048, 8192], P(None, 'tp')
- w_down: bfloat16 [8192, 2048], P('tp')
Outputs:
- output 1: bfloat16 [128, 2048], P('dp'), parts along dimension 0
- output 2: bfloat16 [128, 512, 16, 128], P('dp', 'sp', 'tp'), parts along dimension 0
- output 3: bfloat16 [128, 512, 16, 128], P('dp', 'sp', 'tp'), parts along dimension 0
There are 2 independent parts. The reference program is written for one: setup_inputs(seed, part) draws one part's arguments, and reference() takes and returns one part's arrays. A program takes and returns all parts, laid end to end along the dimension named above; an argument that names none is the same for every part.
All inputs are finite; a program needn't handle non-finite values.
Results may differ from the reference program's by a relative error of at most 0.00593826.
Values sent between devices are 32-bit elements.
A program may use at most 1 GiB of HBM per device.

```python
import jax
import jax.numpy as jnp
from jax import lax

BATCH = 64
CACHE_LEN = 512
BLOCK_LEN = 128
D = 2048
HEADS = 16
HEAD = 128
FF = 8192
PLANT_GAP = 64

NUM_BLOCKS = CACHE_LEN // BLOCK_LEN
LN_EPS = 1e-5
ALIBI_CAP = 256.0


def layer_norm(x_f32, gain):
    mean = jnp.mean(x_f32, axis=-1, keepdims=True)
    centred = x_f32 - mean
    variance = jnp.mean(centred * centred, axis=-1, keepdims=True)
    return centred * lax.rsqrt(variance + LN_EPS) * gain


def alibi_slopes():
    return jnp.exp2(-8.0 * (jnp.arange(HEADS).astype(jnp.float32) + 1.0) / HEADS)


def setup_inputs(seed: int = 0, part: int = 0) -> dict:
    root = jax.random.key(seed)
    shared = jax.random.split(root, 6)
    own = jax.random.split(jax.random.fold_in(root, part), 7)
    x_in = jax.random.normal(own[0], (BATCH, D), jnp.float32).astype(jnp.bfloat16)
    ln1_gain = jax.random.uniform(shared[0], (D,), jnp.float32, minval=0.5, maxval=1.5)
    w_qkv = (jax.random.normal(shared[1], (D, 3, HEADS, HEAD), jnp.float32) * D ** -0.5).astype(jnp.bfloat16)
    w_out = (jax.random.normal(shared[2], (HEADS, HEAD, D), jnp.float32) * D ** -0.5).astype(jnp.bfloat16)
    ln2_gain = jax.random.uniform(shared[3], (D,), jnp.float32, minval=0.5, maxval=1.5)
    w_up = (jax.random.normal(shared[4], (D, FF), jnp.float32) * D ** -0.5).astype(jnp.bfloat16)
    w_down = (jax.random.normal(shared[5], (FF, D), jnp.float32) * FF ** -0.5).astype(jnp.bfloat16)
    seq_lens = jax.random.randint(own[1], (BATCH,), 1, CACHE_LEN)
    longest = jax.random.randint(own[2], (), 0, BATCH)
    seq_lens = jnp.where(jnp.arange(BATCH) == longest, CACHE_LEN - 1, seq_lens).astype(jnp.int32)
    normed = layer_norm(x_in.astype(jnp.float32), ln1_gain).astype(jnp.bfloat16)
    query = jnp.dot(normed, w_qkv[:, 0].reshape(D, D), preferred_element_type=jnp.float32)
    query = query.astype(jnp.bfloat16).astype(jnp.float32).reshape(BATCH, HEADS, HEAD)
    offsets = jax.random.randint(own[3], (BATCH, CACHE_LEN // PLANT_GAP, 1), 0, PLANT_GAP)
    slot_pos = jnp.arange(CACHE_LEN)
    planted = (jnp.arange(PLANT_GAP)[None, None, :] == offsets).reshape(BATCH, CACHE_LEN)
    planted = planted & (slot_pos[None, :] < seq_lens[:, None])
    gumbel_u = jax.random.uniform(own[4], (BATCH, CACHE_LEN, HEADS), jnp.float32, minval=1e-6, maxval=1.0)
    bonus = 4.0 - 1.5 * jnp.log(-jnp.log(gumbel_u))
    distance = (seq_lens[:, None] - slot_pos[None, :]).astype(jnp.float32)
    target = jnp.minimum(alibi_slopes()[None, None, :] * distance[:, :, None], ALIBI_CAP) + bonus

    def make_keys(args):
        seq_key, q_row, target_row, planted_row = args
        k_rand = jax.random.normal(seq_key, (CACHE_LEN, HEADS, HEAD), jnp.float32)
        along = jnp.einsum("hk,thk->th", q_row, k_rand)
        coef = (target_row * HEAD ** 0.5 - along) / jnp.sum(q_row * q_row, axis=-1)[None, :]
        lifted = k_rand + coef[:, :, None] * q_row[None, :, :]
        return jnp.where(planted_row[:, None, None], lifted, k_rand).astype(jnp.bfloat16)

    def make_values(seq_key):
        return jax.random.normal(seq_key, (CACHE_LEN, HEADS, HEAD), jnp.float32).astype(jnp.bfloat16)

    k_cache = lax.map(make_keys, (jax.random.split(own[5], BATCH), query, target, planted))
    v_cache = lax.map(make_values, jax.random.split(own[6], BATCH))
    return {"x_in": x_in, "seq_lens": seq_lens, "k_cache": k_cache, "v_cache": v_cache, "ln1_gain": ln1_gain, "w_qkv": w_qkv, "w_out": w_out, "ln2_gain": ln2_gain, "w_up": w_up, "w_down": w_down}


def reference(x_in, seq_lens, k_cache, v_cache, ln1_gain, w_qkv, w_out, ln2_gain, w_up, w_down):
    normed = layer_norm(x_in.astype(jnp.float32), ln1_gain).astype(jnp.bfloat16)
    qkv_proj = jnp.dot(normed, w_qkv.reshape(D, 3 * D), preferred_element_type=jnp.float32)
    qkv_proj = qkv_proj.astype(jnp.bfloat16).reshape(BATCH, 3, HEADS, HEAD)
    slot_pos = jnp.arange(CACHE_LEN)
    slot_hit = (slot_pos[None, :] == seq_lens[:, None])[:, :, None, None]
    k_next = jnp.where(slot_hit, qkv_proj[:, 1][:, None], k_cache)
    v_next = jnp.where(slot_hit, qkv_proj[:, 2][:, None], v_cache)
    slopes = alibi_slopes()

    def attend(args):
        q_row, k_seq, v_seq, length = args
        q_f32 = q_row.astype(jnp.float32)

        def block_scores(k_block):
            return jnp.einsum("hk,thk->ht", q_f32, k_block.astype(jnp.float32))

        scores = lax.map(block_scores, k_seq.reshape(NUM_BLOCKS, BLOCK_LEN, HEADS, HEAD))
        scores = jnp.transpose(scores, (1, 0, 2)).reshape(HEADS, CACHE_LEN) * HEAD ** -0.5
        scores = scores - slopes[:, None] * (length - slot_pos).astype(jnp.float32)[None, :]
        scores = jnp.where((slot_pos <= length)[None, :], scores, -jnp.inf)
        row_max = jnp.max(scores, axis=1, keepdims=True)
        weights = jnp.exp(scores - row_max)
        row_sum = jnp.sum(weights, axis=1)
        weights_b = weights.astype(jnp.bfloat16).astype(jnp.float32)
        weights_b = jnp.transpose(weights_b.reshape(HEADS, NUM_BLOCKS, BLOCK_LEN), (1, 0, 2))

        def block_sum(carry, block_pair):
            w_block, v_block = block_pair
            return carry + jnp.einsum("ht,thk->hk", w_block, v_block.astype(jnp.float32)), None

        summed, _ = lax.scan(block_sum, jnp.zeros((HEADS, HEAD), jnp.float32), (weights_b, v_seq.reshape(NUM_BLOCKS, BLOCK_LEN, HEADS, HEAD)))
        return summed / row_sum[:, None]

    attended = lax.map(attend, (qkv_proj[:, 0], k_next, v_next, seq_lens))
    attended = attended.astype(jnp.bfloat16).reshape(BATCH, D)
    residual = x_in.astype(jnp.float32) + jnp.dot(attended, w_out.reshape(D, D), preferred_element_type=jnp.float32)
    normed_mid = layer_norm(residual, ln2_gain).astype(jnp.bfloat16)
    hidden = jax.nn.gelu(jnp.dot(normed_mid, w_up, preferred_element_type=jnp.float32), approximate=False).astype(jnp.bfloat16)
    x_out = (residual + jnp.dot(hidden, w_down, preferred_element_type=jnp.float32)).astype(jnp.bfloat16)
    return (x_out, k_next, v_next)
```

```python
import functools

import jax
import jax.numpy as jnp
from jax import lax
from jax.experimental import pallas as pl
from jax.experimental.pallas import tpu as pltpu
from jax.sharding import PartitionSpec as P

LN_EPS = 1e-5
MESH = pl.DeviceIdType.MESH


def layer_norm(x_f32, gain):
    mean = jnp.mean(x_f32, axis=-1, keepdims=True)
    centred = x_f32 - mean
    variance = jnp.mean(centred * centred, axis=-1, keepdims=True)
    return centred * lax.rsqrt(variance + LN_EPS) * gain


def gelu(x):
    return 0.5 * x * (1.0 + lax.erf(x * (0.5 ** 0.5)))


def tail_kernel(tp, sp, heads, hd, pay_ref, x_ref, gain_ref, wo_hbm, wu_hbm, wd_hbm, out_ref,
                wo, wu, wd, got_pay, part, got_part, r_all, h_mid, hidden, down, got_down, x_all,
                wo_sem, wu_sem, wd_sem, s1, r1, s2, r2, s3, r3, s4, r4, s5z, s5y, s5c, r5):
    my_tp = lax.axis_index("tp")
    my_sp = lax.axis_index("sp")
    rows = x_ref.shape[0] // sp
    cols = x_ref.shape[1] // tp

    barrier = pltpu.get_barrier_semaphore()
    for off in range(1, sp):
        pl.semaphore_signal(barrier, inc=1, device_id={"sp": lax.rem(my_sp + off, sp)}, device_id_type=MESH)
    for off in range(1, tp):
        pl.semaphore_signal(barrier, inc=1, device_id={"tp": lax.rem(my_tp + off, tp)}, device_id_type=MESH)

    loads = {}
    for name, src, dst, sem in (("o", wo_hbm, wo, wo_sem), ("u", wu_hbm, wu, wu_sem), ("d", wd_hbm, wd, wd_sem)):
        for j in range(tp):
            copy = pltpu.make_async_copy(src.at[:, pl.ds(j * cols, cols)], dst.at[j], sem.at[j])
            copy.start()
            loads[name, j] = copy

    pl.semaphore_wait(barrier, sp + tp - 2)

    sends = []
    for off in range(1, sp):
        peer = lax.rem(my_sp + off, sp)
        copy = pltpu.make_async_remote_copy(
            pay_ref.at[pl.ds(pl.multiple_of(peer * rows, rows), rows)], got_pay.at[my_sp],
            s1.at[off], r1.at[my_sp], device_id={"sp": peer}, device_id_type=MESH)
        copy.start()
        sends.append(copy)

    def arrived(dst, sem):
        pltpu.make_async_copy(dst, dst, sem).wait()

    blocks = [pay_ref[pl.ds(pl.multiple_of(my_sp * rows, rows), rows), :]]
    for off in range(1, sp):
        peer = lax.rem(my_sp + off, sp)
        arrived(got_pay.at[peer], r1.at[peer])
        blocks.append(got_pay[peer])
    width = heads * hd
    stats = [b[:, width:] for b in blocks]
    top = functools.reduce(jnp.maximum, stats)
    scale = [jnp.exp(s - top) for s in stats]
    attended = []
    for h in range(heads):
        num = sum(c[:, h:h + 1] * b[:, h * hd:(h + 1) * hd] for c, b in zip(scale, blocks))
        den = sum(c[:, h:h + 1] * s[:, heads + h:heads + h + 1] for c, s in zip(scale, stats))
        attended.append(num / den)
    attended = jnp.concatenate(attended, axis=1).astype(jnp.bfloat16)

    for j in range(tp):
        loads["o", j].wait()
    for off in range(1, tp):
        peer = lax.rem(my_tp + off, tp)
        part[peer] = jnp.dot(attended, wo[peer], preferred_element_type=jnp.float32)
        copy = pltpu.make_async_remote_copy(part.at[peer], got_part.at[my_tp], s2.at[off], r2.at[my_tp],
                                            device_id={"tp": peer}, device_id_type=MESH)
        copy.start()
        sends.append(copy)
    mine = jnp.dot(attended, wo[my_tp], preferred_element_type=jnp.float32)
    row0 = pl.multiple_of(my_sp * rows, rows)
    mine += x_ref[pl.ds(row0, rows), pl.ds(pl.multiple_of(my_tp * cols, cols), cols)].astype(jnp.float32)
    for off in range(1, tp):
        peer = lax.rem(my_tp + off, tp)
        arrived(got_part.at[peer], r2.at[peer])
        mine += got_part[peer]
    r_all[my_tp] = mine
    for off in range(1, tp):
        peer = lax.rem(my_tp + off, tp)
        copy = pltpu.make_async_remote_copy(r_all.at[my_tp], r_all.at[my_tp], s3.at[off], r3.at[my_tp],
                                            device_id={"tp": peer}, device_id_type=MESH)
        copy.start()
        sends.append(copy)
    for off in range(1, tp):
        peer = lax.rem(my_tp + off, tp)
        arrived(r_all.at[peer], r3.at[peer])

    r = jnp.concatenate([r_all[j] for j in range(tp)], axis=1)
    h_mid[...] = layer_norm(r, gain_ref[...]).astype(jnp.bfloat16)

    for j in range(tp):
        loads["u", j].wait()
        up = jnp.dot(h_mid[...], wu[j], preferred_element_type=jnp.float32)
        hidden[:, j * cols:(j + 1) * cols] = gelu(up).astype(jnp.bfloat16)

    for j in range(tp):
        loads["d", j].wait()
    for off in range(1, tp):
        peer = lax.rem(my_tp + off, tp)
        down[peer] = jnp.dot(hidden[...], wd[peer], preferred_element_type=jnp.float32)
        copy = pltpu.make_async_remote_copy(down.at[peer], got_down.at[my_tp], s4.at[off], r4.at[my_tp],
                                            device_id={"tp": peer}, device_id_type=MESH)
        copy.start()
        sends.append(copy)
    mine = r_all[my_tp] + jnp.dot(hidden[...], wd[my_tp], preferred_element_type=jnp.float32)
    for off in range(1, tp):
        peer = lax.rem(my_tp + off, tp)
        arrived(got_down.at[peer], r4.at[peer])
        mine += got_down[peer]
    x_all[my_sp, my_tp] = mine.astype(jnp.bfloat16).astype(jnp.float32)

    side = lax.rem(my_sp + 2, sp)
    twin = my_sp + 1 - 2 * lax.rem(my_sp, 2)
    side_twin = lax.rem(twin + 2, sp)

    def pass_on(s, t, send_sem, slot, to):
        copy = pltpu.make_async_remote_copy(x_all.at[s, t], x_all.at[s, t], send_sem.at[slot], r5.at[s, t],
                                            device_id=to, device_id_type=MESH)
        copy.start()
        sends.append(copy)

    for off in range(1, tp):
        pass_on(my_sp, my_tp, s5z, off, {"tp": lax.rem(my_tp + off, tp)})
    pass_on(my_sp, my_tp, s5y, 0, {"sp": side})
    pass_on(my_sp, my_tp, s5c, 0, {"sp": twin})
    for off in range(1, tp):
        peer = lax.rem(my_tp + off, tp)
        arrived(x_all.at[my_sp, peer], r5.at[my_sp, peer])
        pass_on(my_sp, peer, s5y, off, {"sp": side})
        pass_on(my_sp, peer, s5c, off, {"sp": twin})
    for off in range(tp):
        peer = lax.rem(my_tp + off, tp)
        arrived(x_all.at[side, peer], r5.at[side, peer])
        pass_on(side, peer, s5c, tp + off, {"sp": twin})
    for who in (twin, side_twin):
        for off in range(tp):
            peer = lax.rem(my_tp + off, tp)
            arrived(x_all.at[who, peer], r5.at[who, peer])
    for s in range(sp):
        for t in range(tp):
            out_ref[s * rows:(s + 1) * rows, t * cols:(t + 1) * cols] = x_all[s, t].astype(jnp.bfloat16)
    for copy in sends:
        copy.wait_send()


def tail(tp, sp, heads, hd, pay, x_in, gain, w_out, w_up, w_down):
    batch, d = x_in.shape
    rows, cols = batch // sp, d // tp
    ff = w_up.shape[1]
    width = heads * hd
    vmem = pl.BlockSpec(memory_space=pltpu.VMEM)
    hbm = pl.BlockSpec(memory_space=pl.ANY)
    dma = pltpu.SemaphoreType.DMA
    return pl.pallas_call(
        functools.partial(tail_kernel, tp, sp, heads, hd),
        out_shape=jax.ShapeDtypeStruct((batch, d), jnp.bfloat16),
        in_specs=[vmem, vmem, vmem, hbm, hbm, hbm],
        out_specs=vmem,
        scratch_shapes=[
            pltpu.VMEM((tp, width, cols), jnp.bfloat16),
            pltpu.VMEM((tp, d, ff // tp), jnp.bfloat16),
            pltpu.VMEM((tp, ff, cols), jnp.bfloat16),
            pltpu.VMEM((sp, rows, pay.shape[1]), jnp.float32),
            pltpu.VMEM((tp, rows, cols), jnp.float32),
            pltpu.VMEM((tp, rows, cols), jnp.float32),
            pltpu.VMEM((tp, rows, cols), jnp.float32),
            pltpu.VMEM((rows, d), jnp.bfloat16),
            pltpu.VMEM((rows, ff), jnp.bfloat16),
            pltpu.VMEM((tp, rows, cols), jnp.float32),
            pltpu.VMEM((tp, rows, cols), jnp.float32),
            pltpu.VMEM((sp, tp, rows, cols), jnp.float32),
            dma((tp,)), dma((tp,)), dma((tp,)),
            dma((sp,)), dma((sp,)), dma((tp,)), dma((tp,)), dma((tp,)), dma((tp,)), dma((tp,)), dma((tp,)),
            dma((tp,)), dma((tp,)), dma((2 * tp,)), dma((sp, tp)),
        ],
        compiler_params=pltpu.CompilerParams(collective_id=0, has_side_effects=True, vmem_limit_bytes=32 * 2 ** 20),
        name="tail",
    )(pay, x_in, gain[None, :], w_out.reshape(width, d), w_up, w_down)


def solution(mesh):
    tp_size = mesh.shape["tp"]
    sp_size = mesh.shape["sp"]

    def local_layer(x_in, seq_lens, k_cache, v_cache, ln1_gain, w_qkv, w_out, ln2_gain, w_up, w_down):
        tok_dev = k_cache.shape[1]
        local_heads = k_cache.shape[2]
        head_dim = k_cache.shape[3]
        heads = local_heads * tp_size
        tp_index = lax.axis_index("tp")
        sp_index = lax.axis_index("sp")
        normed = layer_norm(x_in.astype(jnp.float32), ln1_gain).astype(jnp.bfloat16)
        qkv_proj = jnp.einsum("bd,dchk->bchk", normed, w_qkv, preferred_element_type=jnp.float32).astype(jnp.bfloat16)
        slot_pos = sp_index * tok_dev + jnp.arange(tok_dev)
        slot_hit = (slot_pos[None, :] == seq_lens[:, None])[:, :, None, None]
        k_next = jnp.where(slot_hit, qkv_proj[:, 1][:, None], k_cache)
        v_next = jnp.where(slot_hit, qkv_proj[:, 2][:, None], v_cache)
        head_ids = tp_index * local_heads + jnp.arange(local_heads)
        slopes = jnp.exp2(-8.0 * (head_ids + 1).astype(jnp.float32) / heads)
        scores = jnp.einsum("bhk,bthk->bht", qkv_proj[:, 0], k_next, preferred_element_type=jnp.float32) * head_dim ** -0.5
        distance = (seq_lens[:, None] - slot_pos[None, :]).astype(jnp.float32)
        scores = scores - slopes[None, :, None] * distance[:, None, :]
        is_valid = (slot_pos[None, :] <= seq_lens[:, None])[:, None, :]
        scores = jnp.where(is_valid, scores, -1e30)
        local_max = jnp.max(scores, axis=2)
        weights = jnp.where(is_valid, jnp.exp(scores - local_max[:, :, None]), 0.0)
        local_sum = jnp.sum(weights, axis=2)
        local_out = jnp.einsum("bht,bthk->bhk", weights.astype(jnp.bfloat16), v_next, preferred_element_type=jnp.float32)
        batch = x_in.shape[0]
        filler = jnp.zeros((batch, 128 - 2 * local_heads), jnp.float32)
        pay = jnp.concatenate([local_out.reshape(batch, -1), local_max, local_sum, filler], axis=1)
        x_out = tail(tp_size, sp_size, local_heads, head_dim, pay, x_in, ln2_gain, w_out, w_up, w_down)
        return x_out, k_next, v_next

    cache_spec = P("dp", "sp", "tp", None)
    in_specs = (P("dp", None), P("dp"), cache_spec, cache_spec, P(None), P(None, None, "tp", None), P("tp", None, None), P(None), P(None, "tp"), P("tp", None))
    out_specs = (P("dp", None), cache_spec, cache_spec)
    return jax.shard_map(local_layer, mesh=mesh, in_specs=in_specs, out_specs=out_specs, check_vma=False)
```

```python
import functools

import jax
import jax.numpy as jnp
from jax import lax
from jax.experimental import pallas as pl
from jax.experimental.pallas import tpu as pltpu
from jax.sharding import PartitionSpec as P

LN_EPS = 1e-5
MESH = pl.DeviceIdType.MESH


def layer_norm(x_f32, gain):
    mean = jnp.mean(x_f32, axis=-1, keepdims=True)
    centred = x_f32 - mean
    variance = jnp.mean(centred * centred, axis=-1, keepdims=True)
    return centred * lax.rsqrt(variance + LN_EPS) * gain


def gelu(x):
    return 0.5 * x * (1.0 + lax.erf(x * (0.5 ** 0.5)))


def tail_kernel(tp, sp, heads, hd, pay_ref, x_ref, gain_ref, wo_hbm, wu_hbm, wd_hbm, out_ref,
                wo, wu, wd, got_pay, att, part, got_part, r_all, h_mid, hidden, down, got_down, x_all,
                wo_sem, wu_sem, wd_sem, s1, r1, s2, r2, s3, r3, s4, r4, s5z, s5y, s5c, r5):
    my_tp = lax.axis_index("tp")
    my_sp = lax.axis_index("sp")
    rows = x_ref.shape[0] // sp
    cols = x_ref.shape[1] // tp

    barrier = pltpu.get_barrier_semaphore()
    for off in range(1, sp):
        pl.semaphore_signal(barrier, inc=1, device_id={"sp": lax.rem(my_sp + off, sp)}, device_id_type=MESH)
    for off in range(1, tp):
        pl.semaphore_signal(barrier, inc=1, device_id={"tp": lax.rem(my_tp + off, tp)}, device_id_type=MESH)

    loads = {}
    for name, src, dst, sem in (("o", wo_hbm, wo, wo_sem), ("u", wu_hbm, wu, wu_sem), ("d", wd_hbm, wd, wd_sem)):
        for j in range(tp):
            copy = pltpu.make_async_copy(src.at[:, pl.ds(j * cols, cols)], dst.at[j], sem.at[j])
            copy.start()
            loads[name, j] = copy

    pl.semaphore_wait(barrier, sp + tp - 2)

    sends = []
    for off in range(1, sp):
        peer = lax.rem(my_sp + off, sp)
        copy = pltpu.make_async_remote_copy(
            pay_ref.at[peer], got_pay.at[my_sp],
            s1.at[off], r1.at[my_sp], device_id={"sp": peer}, device_id_type=MESH)
        copy.start()
        sends.append(copy)

    def arrived(dst, sem):
        pltpu.make_async_copy(dst, dst, sem).wait()

    pairs = rows * heads
    blocks = [pay_ref[my_sp]]
    for off in range(1, sp):
        peer = lax.rem(my_sp + off, sp)
        arrived(got_pay.at[peer], r1.at[peer])
        blocks.append(got_pay[peer])
    top = functools.reduce(jnp.maximum, [b[pairs:pairs + 1] for b in blocks])
    scale = [jnp.exp(b[pairs:pairs + 1] - top) for b in blocks]
    den = sum(c * b[pairs + 1:pairs + 2] for c, b in zip(scale, blocks))
    coef = jnp.concatenate(scale + [den] * (8 - sp), axis=0).T
    coef = jnp.where(lax.rem(my_sp, 2) == 0, coef[:pairs], coef[pairs:])
    att[...] = sum(coef[:, i:i + 1] * b[:pairs] for i, b in enumerate(blocks)) / coef[:, sp:sp + 1]
    attended = jnp.concatenate([att[pl.ds(h, rows, stride=heads), :] for h in range(heads)], axis=1).astype(jnp.bfloat16)

    for j in range(tp):
        loads["o", j].wait()
    for off in range(1, tp):
        peer = lax.rem(my_tp + off, tp)
        part[peer] = jnp.dot(attended, wo[peer], preferred_element_type=jnp.float32)
        copy = pltpu.make_async_remote_copy(part.at[peer], got_part.at[my_tp], s2.at[off], r2.at[my_tp],
                                            device_id={"tp": peer}, device_id_type=MESH)
        copy.start()
        sends.append(copy)
    mine = jnp.dot(attended, wo[my_tp], preferred_element_type=jnp.float32)
    row0 = pl.multiple_of(my_sp * rows, rows)
    mine += x_ref[pl.ds(row0, rows), pl.ds(pl.multiple_of(my_tp * cols, cols), cols)].astype(jnp.float32)
    for off in range(1, tp):
        peer = lax.rem(my_tp + off, tp)
        arrived(got_part.at[peer], r2.at[peer])
        mine += got_part[peer]
    r_all[my_tp] = mine
    for off in range(1, tp):
        peer = lax.rem(my_tp + off, tp)
        copy = pltpu.make_async_remote_copy(r_all.at[my_tp], r_all.at[my_tp], s3.at[off], r3.at[my_tp],
                                            device_id={"tp": peer}, device_id_type=MESH)
        copy.start()
        sends.append(copy)
    for off in range(1, tp):
        peer = lax.rem(my_tp + off, tp)
        arrived(r_all.at[peer], r3.at[peer])

    r = jnp.concatenate([r_all[j] for j in range(tp)], axis=1)
    h_mid[...] = layer_norm(r, gain_ref[...]).astype(jnp.bfloat16)

    for j in range(tp):
        loads["u", j].wait()
        up = jnp.dot(h_mid[...], wu[j], preferred_element_type=jnp.float32)
        hidden[:, j * cols:(j + 1) * cols] = gelu(up).astype(jnp.bfloat16)

    for j in range(tp):
        loads["d", j].wait()
    for off in range(1, tp):
        peer = lax.rem(my_tp + off, tp)
        down[peer] = jnp.dot(hidden[...], wd[peer], preferred_element_type=jnp.float32)
        copy = pltpu.make_async_remote_copy(down.at[peer], got_down.at[my_tp], s4.at[off], r4.at[my_tp],
                                            device_id={"tp": peer}, device_id_type=MESH)
        copy.start()
        sends.append(copy)
    mine = r_all[my_tp] + jnp.dot(hidden[...], wd[my_tp], preferred_element_type=jnp.float32)
    for off in range(1, tp):
        peer = lax.rem(my_tp + off, tp)
        arrived(got_down.at[peer], r4.at[peer])
        mine += got_down[peer]
    x_all[my_sp, my_tp] = mine.astype(jnp.bfloat16).astype(jnp.float32)

    side = lax.rem(my_sp + 2, sp)
    twin = my_sp + 1 - 2 * lax.rem(my_sp, 2)
    side_twin = lax.rem(twin + 2, sp)

    def pass_on(s, t, send_sem, slot, to):
        copy = pltpu.make_async_remote_copy(x_all.at[s, t], x_all.at[s, t], send_sem.at[slot], r5.at[s, t],
                                            device_id=to, device_id_type=MESH)
        copy.start()
        sends.append(copy)

    for off in range(1, tp):
        pass_on(my_sp, my_tp, s5z, off, {"tp": lax.rem(my_tp + off, tp)})
    pass_on(my_sp, my_tp, s5y, 0, {"sp": side})
    pass_on(my_sp, my_tp, s5c, 0, {"sp": twin})
    for off in range(1, tp):
        peer = lax.rem(my_tp + off, tp)
        arrived(x_all.at[my_sp, peer], r5.at[my_sp, peer])
        pass_on(my_sp, peer, s5y, off, {"sp": side})
        pass_on(my_sp, peer, s5c, off, {"sp": twin})
    for off in range(tp):
        peer = lax.rem(my_tp + off, tp)
        arrived(x_all.at[side, peer], r5.at[side, peer])
        pass_on(side, peer, s5c, tp + off, {"sp": twin})
    for who in (twin, side_twin):
        for off in range(tp):
            peer = lax.rem(my_tp + off, tp)
            arrived(x_all.at[who, peer], r5.at[who, peer])
    for s in range(sp):
        for t in range(tp):
            out_ref[s * rows:(s + 1) * rows, t * cols:(t + 1) * cols] = x_all[s, t].astype(jnp.bfloat16)
    for copy in sends:
        copy.wait_send()


def tail(tp, sp, heads, hd, pay, x_in, gain, w_out, w_up, w_down):
    batch, d = x_in.shape
    rows, cols = batch // sp, d // tp
    ff = w_up.shape[1]
    width = heads * hd
    vmem = pl.BlockSpec(memory_space=pltpu.VMEM)
    hbm = pl.BlockSpec(memory_space=pl.ANY)
    dma = pltpu.SemaphoreType.DMA
    return pl.pallas_call(
        functools.partial(tail_kernel, tp, sp, heads, hd),
        out_shape=jax.ShapeDtypeStruct((batch, d), jnp.bfloat16),
        in_specs=[vmem, vmem, vmem, hbm, hbm, hbm],
        out_specs=vmem,
        scratch_shapes=[
            pltpu.VMEM((tp, width, cols), jnp.bfloat16),
            pltpu.VMEM((tp, d, ff // tp), jnp.bfloat16),
            pltpu.VMEM((tp, ff, cols), jnp.bfloat16),
            pltpu.VMEM(pay.shape, jnp.float32),
            pltpu.VMEM((rows * heads, hd), jnp.float32),
            pltpu.VMEM((tp, rows, cols), jnp.float32),
            pltpu.VMEM((tp, rows, cols), jnp.float32),
            pltpu.VMEM((tp, rows, cols), jnp.float32),
            pltpu.VMEM((rows, d), jnp.bfloat16),
            pltpu.VMEM((rows, ff), jnp.bfloat16),
            pltpu.VMEM((tp, rows, cols), jnp.float32),
            pltpu.VMEM((tp, rows, cols), jnp.float32),
            pltpu.VMEM((sp, tp, rows, cols), jnp.float32),
            dma((tp,)), dma((tp,)), dma((tp,)),
            dma((sp,)), dma((sp,)), dma((tp,)), dma((tp,)), dma((tp,)), dma((tp,)), dma((tp,)), dma((tp,)),
            dma((tp,)), dma((tp,)), dma((2 * tp,)), dma((sp, tp)),
        ],
        compiler_params=pltpu.CompilerParams(collective_id=0, has_side_effects=True, vmem_limit_bytes=60 * 2 ** 20),
        name="tail",
    )(pay, x_in, gain[None, :], w_out.reshape(width, d), w_up, w_down)


def attend_kernel(lens_ref, qkv_ref, k_hbm, v_hbm, pay_ref, kn_hbm, vn_hbm,
                  kbuf, vbuf, rep_k, rep_v, p_t, k_in, v_in, k_out, v_out, *, heads, all_heads, sp, chunks):
    batch, pairs, hd = kbuf.shape
    slots = pairs // heads
    per = batch // chunks
    base = lax.axis_index("sp") * slots

    def moves(src, dst, sem, c):
        part = pl.ds(c * per, per)
        return pltpu.make_async_copy(src.at[part], dst.at[part], sem.at[c])

    for c in range(chunks):
        moves(k_hbm, kbuf, k_in, c).start()
    for c in range(chunks):
        moves(v_hbm, vbuf, v_in, c).start()

    low = lax.broadcasted_iota(jnp.int32, (1, 8, hd), 1) < heads
    for rep, i in ((rep_k, 1), (rep_v, 2)):
        new = qkv_ref[i].reshape(batch // 2, 8, hd)
        turned = pltpu.roll(new, heads, 1)
        rep[:, 0] = jnp.where(low, new, turned)
        rep[:, 1] = jnp.where(low, turned, new)

    row_slot = lax.broadcasted_iota(jnp.int32, (16, hd), 0) // heads

    def put_rows(buf, rep, c):
        for b in range(c * per, (c + 1) * per):
            slot = lens_ref[b] - base

            @pl.when((slot >= 0) & (slot < slots))
            def _():
                span = pl.ds(pl.multiple_of(slot // 4 * 16, 16), 16)
                old = buf[b, span, :].astype(jnp.float32)
                new = jnp.concatenate([rep[b // 2, b % 2]] * 2, axis=0)
                buf[b, span, :] = jnp.where(row_slot == lax.rem(slot, 4), new, old).astype(buf.dtype)

    q_t = qkv_ref[0].T.astype(jnp.bfloat16)
    lane = lax.broadcasted_iota(jnp.int32, (1, 128), 1)
    lane_seq, lane_head = lane // heads, lax.rem(lane, heads)
    group = 128 // heads
    row = lax.broadcasted_iota(jnp.int32, (pairs, 128), 0)
    pos = base + row // heads
    same_head = lax.rem(row, heads) == lane_head
    slope = jnp.exp2((lax.axis_index("tp") * heads + lane_head + 1).astype(jnp.float32) * (-8.0 / all_heads))
    per_group = chunks // (batch // group)
    for g in range(batch // group):
        q_g = q_t[:, g * 128:(g + 1) * 128]
        scores = None
        for c in range(g * per_group, (g + 1) * per_group):
            moves(k_hbm, kbuf, k_in, c).wait()
            put_rows(kbuf, rep_k, c)
            seqs = range(c * per, (c + 1) * per)
            keys = jnp.concatenate([kbuf[b] for b in seqs], axis=1)
            query = jnp.concatenate([jnp.where(lane_seq == b - g * group, q_g, 0) for b in seqs], axis=0)
            part = jnp.dot(keys, query, preferred_element_type=jnp.float32)
            scores = part if scores is None else scores + part
            moves(kbuf, kn_hbm, k_out, c).start()
        length = jnp.zeros((1, 128), jnp.int32)
        for i in range(group):
            length = jnp.where(lane_seq == i, lens_ref[g * group + i], length)
        scores = scores * hd ** -0.5 - slope * (length - pos).astype(jnp.float32)
        valid = same_head & (pos <= length)
        scores = jnp.where(valid, scores, -1e30)
        top = jnp.max(scores, axis=0, keepdims=True)
        p = jnp.where(valid, jnp.exp(scores - top), 0.0)
        total = jnp.sum(p, axis=0, keepdims=True)
        stats = jnp.concatenate([top, total, jnp.zeros((6, 128), jnp.float32)], axis=0)
        for s in range(g * sp // (batch // group), (g + 1) * sp // (batch // group)):
            pay_ref[s, batch // sp * heads:, :] = stats
        p_t[g * 128:(g + 1) * 128, :] = p.T.astype(jnp.bfloat16)

    quad = 16 // heads
    row_seq = lax.broadcasted_iota(jnp.int32, (16, hd), 0) // heads
    for c in range(chunks):
        moves(v_hbm, vbuf, v_in, c).wait()
        put_rows(vbuf, rep_v, c)
        for b in range(c * per, (c + 1) * per, quad):
            values = jnp.concatenate([vbuf[b + i] for i in range(quad)], axis=1)
            out = jnp.dot(p_t[b * heads:b * heads + 16, :], values, preferred_element_type=jnp.float32)
            out = sum(jnp.where(row_seq == i, out[:, i * hd:(i + 1) * hd], 0.0) for i in range(quad))
            owner = b * sp // batch
            at = (b - owner * (batch // sp)) * heads
            pay_ref[owner, at:at + 16, :] = out
        moves(vbuf, vn_hbm, v_out, c).start()
    for c in range(chunks):
        moves(kbuf, kn_hbm, k_out, c).wait()
        moves(vbuf, vn_hbm, v_out, c).wait()


def attend(tp, sp, lens, qkv, k_cache, v_cache):
    batch, slots, heads, hd = k_cache.shape
    chunks = 8
    flat = (batch, slots * heads, hd)
    vmem = pl.BlockSpec(memory_space=pltpu.VMEM)
    hbm = pl.BlockSpec(memory_space=pl.ANY)
    dma = pltpu.SemaphoreType.DMA
    pay, k_next, v_next = pl.pallas_call(
        functools.partial(attend_kernel, heads=heads, all_heads=heads * tp, sp=sp, chunks=chunks),
        out_shape=(jax.ShapeDtypeStruct((sp, batch // sp * heads + 8, hd), jnp.float32),
                   jax.ShapeDtypeStruct(flat, k_cache.dtype), jax.ShapeDtypeStruct(flat, v_cache.dtype)),
        in_specs=[pl.BlockSpec(memory_space=pltpu.SMEM), vmem, hbm, hbm],
        out_specs=(vmem, hbm, hbm),
        scratch_shapes=[
            pltpu.VMEM(flat, k_cache.dtype), pltpu.VMEM(flat, v_cache.dtype),
            pltpu.VMEM((batch // 2, 2, 8, hd), jnp.float32), pltpu.VMEM((batch // 2, 2, 8, hd), jnp.float32),
            pltpu.VMEM((batch * heads, slots * heads), jnp.bfloat16),
            dma((chunks,)), dma((chunks,)), dma((chunks,)), dma((chunks,)),
        ],
        compiler_params=pltpu.CompilerParams(vmem_limit_bytes=60 * 2 ** 20),
        name="attend",
    )(lens, qkv, k_cache.reshape(flat), v_cache.reshape(flat))
    return pay, k_next.reshape(k_cache.shape), v_next.reshape(v_cache.shape)


def solution(mesh):
    tp_size = mesh.shape["tp"]
    sp_size = mesh.shape["sp"]

    def local_layer(x_in, seq_lens, k_cache, v_cache, ln1_gain, w_qkv, w_out, ln2_gain, w_up, w_down):
        batch = x_in.shape[0]
        local_heads = k_cache.shape[2]
        head_dim = k_cache.shape[3]
        normed = layer_norm(x_in.astype(jnp.float32), ln1_gain).astype(jnp.bfloat16)
        qkv_proj = jnp.einsum("bd,dchk->cbhk", normed, w_qkv, preferred_element_type=jnp.float32).astype(jnp.bfloat16)
        qkv_proj = qkv_proj.astype(jnp.float32).reshape(3, batch * local_heads, head_dim)
        pay, k_next, v_next = attend(tp_size, sp_size, seq_lens, qkv_proj, k_cache, v_cache)
        x_out = tail(tp_size, sp_size, local_heads, head_dim, pay, x_in, ln2_gain, w_out, w_up, w_down)
        return x_out, k_next, v_next

    cache_spec = P("dp", "sp", "tp", None)
    in_specs = (P("dp", None), P("dp"), cache_spec, cache_spec, P(None), P(None, None, "tp", None), P("tp", None, None), P(None), P(None, "tp"), P("tp", None))
    out_specs = (P("dp", None), cache_spec, cache_spec)
    return jax.shard_map(local_layer, mesh=mesh, in_specs=in_specs, out_specs=out_specs, check_vma=False)
```

```python
import functools

import jax
import jax.numpy as jnp
from jax import lax
from jax.experimental import pallas as pl
from jax.experimental.pallas import tpu as pltpu
from jax.sharding import PartitionSpec as P

LN_EPS = 1e-5
MESH = pl.DeviceIdType.MESH


def layer_norm(x_f32, gain):
    mean = jnp.mean(x_f32, axis=-1, keepdims=True)
    centred = x_f32 - mean
    variance = jnp.mean(centred * centred, axis=-1, keepdims=True)
    return centred * lax.rsqrt(variance + LN_EPS) * gain


def gelu(x):
    return 0.5 * x * (1.0 + lax.erf(x * (0.5 ** 0.5)))


def tail_kernel(tp, sp, heads, hd, pay_ref, x_ref, gain_ref, wo_hbm, wu_hbm, wd_hbm, out_ref,
                wo, wu, wd, got_pay, att, part, got_part, r_all, h_mid, hidden, down, got_down, x_all,
                wo_sem, wu_sem, wd_sem, s1, r1, s2, r2, s3, r3, s4, r4, s5z, s5y, s5c, r5):
    my_tp = lax.axis_index("tp")
    my_sp = lax.axis_index("sp")
    rows = x_ref.shape[0] // sp
    cols = x_ref.shape[1] // tp

    barrier = pltpu.get_barrier_semaphore()
    for off in range(1, sp):
        pl.semaphore_signal(barrier, inc=1, device_id={"sp": lax.rem(my_sp + off, sp)}, device_id_type=MESH)
    for off in range(1, tp):
        pl.semaphore_signal(barrier, inc=1, device_id={"tp": lax.rem(my_tp + off, tp)}, device_id_type=MESH)

    loads = {}
    for name, src, dst, sem in (("o", wo_hbm, wo, wo_sem), ("u", wu_hbm, wu, wu_sem), ("d", wd_hbm, wd, wd_sem)):
        for j in range(tp):
            copy = pltpu.make_async_copy(src.at[:, pl.ds(j * cols, cols)], dst.at[j], sem.at[j])
            copy.start()
            loads[name, j] = copy

    pl.semaphore_wait(barrier, sp + tp - 2)

    sends = []
    for off in range(1, sp):
        peer = lax.rem(my_sp + off, sp)
        copy = pltpu.make_async_remote_copy(
            pay_ref.at[peer], got_pay.at[my_sp],
            s1.at[off], r1.at[my_sp], device_id={"sp": peer}, device_id_type=MESH)
        copy.start()
        sends.append(copy)

    def arrived(dst, sem):
        pltpu.make_async_copy(dst, dst, sem).wait()

    pairs = rows * heads
    blocks = [pay_ref[my_sp]]
    for off in range(1, sp):
        peer = lax.rem(my_sp + off, sp)
        arrived(got_pay.at[peer], r1.at[peer])
        blocks.append(got_pay[peer])
    top = functools.reduce(jnp.maximum, [b[pairs:pairs + 1] for b in blocks])
    scale = [jnp.exp(b[pairs:pairs + 1] - top) for b in blocks]
    den = sum(c * b[pairs + 1:pairs + 2] for c, b in zip(scale, blocks))
    coef = jnp.concatenate(scale + [den] * (8 - sp), axis=0).T
    coef = jnp.where(lax.rem(my_sp, 2) == 0, coef[:pairs], coef[pairs:])
    att[...] = sum(coef[:, i:i + 1] * b[:pairs] for i, b in enumerate(blocks)) / coef[:, sp:sp + 1]
    attended = jnp.concatenate([att[pl.ds(h, rows, stride=heads), :] for h in range(heads)], axis=1).astype(jnp.bfloat16)

    for j in range(tp):
        loads["o", j].wait()
    for off in range(1, tp):
        peer = lax.rem(my_tp + off, tp)
        part[peer] = jnp.dot(attended, wo[peer], preferred_element_type=jnp.float32)
        copy = pltpu.make_async_remote_copy(part.at[peer], got_part.at[my_tp], s2.at[off], r2.at[my_tp],
                                            device_id={"tp": peer}, device_id_type=MESH)
        copy.start()
        sends.append(copy)
    mine = jnp.dot(attended, wo[my_tp], preferred_element_type=jnp.float32)
    row0 = pl.multiple_of(my_sp * rows, rows)
    mine += x_ref[pl.ds(row0, rows), pl.ds(pl.multiple_of(my_tp * cols, cols), cols)].astype(jnp.float32)
    for off in range(1, tp):
        peer = lax.rem(my_tp + off, tp)
        arrived(got_part.at[peer], r2.at[peer])
        mine += got_part[peer]
    r_all[my_tp] = mine
    for off in range(1, tp):
        peer = lax.rem(my_tp + off, tp)
        copy = pltpu.make_async_remote_copy(r_all.at[my_tp], r_all.at[my_tp], s3.at[off], r3.at[my_tp],
                                            device_id={"tp": peer}, device_id_type=MESH)
        copy.start()
        sends.append(copy)
    for off in range(1, tp):
        peer = lax.rem(my_tp + off, tp)
        arrived(r_all.at[peer], r3.at[peer])

    r = jnp.concatenate([r_all[j] for j in range(tp)], axis=1)
    h_mid[...] = layer_norm(r, gain_ref[...]).astype(jnp.bfloat16)

    for j in range(tp):
        loads["u", j].wait()
        up = jnp.dot(h_mid[...], wu[j], preferred_element_type=jnp.float32)
        hidden[:, j * cols:(j + 1) * cols] = gelu(up).astype(jnp.bfloat16)

    for j in range(tp):
        loads["d", j].wait()
    for off in range(1, tp):
        peer = lax.rem(my_tp + off, tp)
        down[peer] = jnp.dot(hidden[...], wd[peer], preferred_element_type=jnp.float32)
        copy = pltpu.make_async_remote_copy(down.at[peer], got_down.at[my_tp], s4.at[off], r4.at[my_tp],
                                            device_id={"tp": peer}, device_id_type=MESH)
        copy.start()
        sends.append(copy)
    mine = r_all[my_tp] + jnp.dot(hidden[...], wd[my_tp], preferred_element_type=jnp.float32)
    for off in range(1, tp):
        peer = lax.rem(my_tp + off, tp)
        arrived(got_down.at[peer], r4.at[peer])
        mine += got_down[peer]
    x_all[my_sp, my_tp] = mine.astype(jnp.bfloat16).astype(jnp.float32)

    side = lax.rem(my_sp + 2, sp)
    twin = my_sp + 1 - 2 * lax.rem(my_sp, 2)
    side_twin = lax.rem(twin + 2, sp)

    def pass_on(s, t, send_sem, slot, to):
        copy = pltpu.make_async_remote_copy(x_all.at[s, t], x_all.at[s, t], send_sem.at[slot], r5.at[s, t],
                                            device_id=to, device_id_type=MESH)
        copy.start()
        sends.append(copy)

    for off in range(1, tp):
        pass_on(my_sp, my_tp, s5z, off, {"tp": lax.rem(my_tp + off, tp)})
    pass_on(my_sp, my_tp, s5y, 0, {"sp": side})
    pass_on(my_sp, my_tp, s5c, 0, {"sp": twin})
    for off in range(1, tp):
        peer = lax.rem(my_tp + off, tp)
        arrived(x_all.at[my_sp, peer], r5.at[my_sp, peer])
        pass_on(my_sp, peer, s5y, off, {"sp": side})
        pass_on(my_sp, peer, s5c, off, {"sp": twin})
    for off in range(tp):
        peer = lax.rem(my_tp + off, tp)
        arrived(x_all.at[side, peer], r5.at[side, peer])
        pass_on(side, peer, s5c, tp + off, {"sp": twin})
    for who in (twin, side_twin):
        for off in range(tp):
            peer = lax.rem(my_tp + off, tp)
            arrived(x_all.at[who, peer], r5.at[who, peer])
    for s in range(sp):
        for t in range(tp):
            out_ref[s * rows:(s + 1) * rows, t * cols:(t + 1) * cols] = x_all[s, t].astype(jnp.bfloat16)
    for copy in sends:
        copy.wait_send()


def tail(tp, sp, heads, hd, pay, x_in, gain, w_out, w_up, w_down):
    batch, d = x_in.shape
    rows, cols = batch // sp, d // tp
    ff = w_up.shape[1]
    width = heads * hd
    vmem = pl.BlockSpec(memory_space=pltpu.VMEM)
    hbm = pl.BlockSpec(memory_space=pltpu.HBM)
    dma = pltpu.SemaphoreType.DMA
    return pl.pallas_call(
        functools.partial(tail_kernel, tp, sp, heads, hd),
        out_shape=jax.ShapeDtypeStruct((batch, d), jnp.bfloat16),
        in_specs=[vmem, vmem, vmem, hbm, hbm, hbm],
        out_specs=vmem,
        scratch_shapes=[
            pltpu.VMEM((tp, width, cols), jnp.bfloat16),
            pltpu.VMEM((tp, d, ff // tp), jnp.bfloat16),
            pltpu.VMEM((tp, ff, cols), jnp.bfloat16),
            pltpu.VMEM(pay.shape, jnp.float32),
            pltpu.VMEM((rows * heads, hd), jnp.float32),
            pltpu.VMEM((tp, rows, cols), jnp.float32),
            pltpu.VMEM((tp, rows, cols), jnp.float32),
            pltpu.VMEM((tp, rows, cols), jnp.float32),
            pltpu.VMEM((rows, d), jnp.bfloat16),
            pltpu.VMEM((rows, ff), jnp.bfloat16),
            pltpu.VMEM((tp, rows, cols), jnp.float32),
            pltpu.VMEM((tp, rows, cols), jnp.float32),
            pltpu.VMEM((sp, tp, rows, cols), jnp.float32),
            dma((tp,)), dma((tp,)), dma((tp,)),
            dma((sp,)), dma((sp,)), dma((tp,)), dma((tp,)), dma((tp,)), dma((tp,)), dma((tp,)), dma((tp,)),
            dma((tp,)), dma((tp,)), dma((2 * tp,)), dma((sp, tp)),
        ],
        compiler_params=pltpu.CompilerParams(collective_id=0, has_side_effects=True, vmem_limit_bytes=24 * 2 ** 20),
        name="tail",
    )(pay, x_in, gain[None, :], *(pltpu.with_memory_space_constraint(w, pltpu.HBM) for w in (w_out.reshape(width, d), w_up, w_down)))


def attend_kernel(lens_hbm, x_hbm, gain_hbm, w_hbm, k_hbm, v_hbm, pay_ref, kn_hbm, vn_hbm,
                  lens_ref, x_ref, gain_ref, wbuf, wide, normed, qkv, kbuf, vbuf, rep_k, rep_v, p_t,
                  small_in, w_in, k_in, v_in, k_out, v_out, *, heads, all_heads, sp, chunks):
    batch, pairs, hd = kbuf.shape
    slots = pairs // heads
    per = batch // chunks
    base = lax.axis_index("sp") * slots

    def moves(src, dst, sem, c):
        part = pl.ds(c * per, per)
        return pltpu.make_async_copy(src.at[part], dst.at[part], sem.at[c])

    small = [pltpu.make_async_copy(src, dst, small_in.at[i])
             for i, (src, dst) in enumerate(((x_hbm, x_ref), (gain_hbm, gain_ref), (lens_hbm, lens_ref)))]
    for copy in small:
        copy.start()
    d = x_ref.shape[1]
    parts = 3 * heads
    depth = wide.shape[0] // parts
    pieces = d // depth
    w_copies = []
    for j in range(pieces):
        part = pl.ds(j * depth * parts, depth * parts)
        w_copies.append(pltpu.make_async_copy(w_hbm.at[part], wbuf.at[part], w_in.at[j]))
        w_copies[j].start()
    moves(k_hbm, kbuf, k_in, 0).start()

    for copy in small:
        copy.wait()
    normed[...] = layer_norm(x_ref[...].astype(jnp.float32), gain_ref[...]).astype(jnp.bfloat16)
    proj = None
    for j in range(pieces):
        w_copies[j].wait()
        if j + 1 < chunks:
            moves(k_hbm, kbuf, k_in, j + 1).start()
        else:
            moves(v_hbm, vbuf, v_in, 0).start()
        wide[...] = wbuf[j * depth * parts:(j + 1) * depth * parts, :].astype(jnp.float32)
        w = jnp.concatenate([wide[pl.ds(i, depth, stride=parts), :].astype(jnp.bfloat16) for i in range(parts)], axis=1)
        part = jnp.dot(normed[:, j * depth:(j + 1) * depth], w, preferred_element_type=jnp.float32)
        proj = part if proj is None else proj + part
    for i in range(parts):
        qkv[i // heads, pl.ds(i % heads, batch, stride=heads), :] = (
            proj[:, i * hd:(i + 1) * hd].astype(jnp.bfloat16).astype(jnp.float32))

    low = lax.broadcasted_iota(jnp.int32, (1, 8, hd), 1) < heads
    for rep, i in ((rep_k, 1), (rep_v, 2)):
        new = qkv[i].reshape(batch // 2, 8, hd)
        turned = pltpu.roll(new, heads, 1)
        rep[:, 0] = jnp.where(low, new, turned)
        rep[:, 1] = jnp.where(low, turned, new)

    row_slot = lax.broadcasted_iota(jnp.int32, (16, hd), 0) // heads

    def put_rows(buf, rep, c):
        for b in range(c * per, (c + 1) * per):
            slot = lens_ref[b] - base

            @pl.when((slot >= 0) & (slot < slots))
            def _():
                span = pl.ds(pl.multiple_of(slot // 4 * 16, 16), 16)
                old = buf[b, span, :].astype(jnp.float32)
                new = jnp.concatenate([rep[b // 2, b % 2]] * 2, axis=0)
                buf[b, span, :] = jnp.where(row_slot == lax.rem(slot, 4), new, old).astype(buf.dtype)

    q_t = qkv[0].T.astype(jnp.bfloat16)
    lane = lax.broadcasted_iota(jnp.int32, (1, 128), 1)
    lane_seq, lane_head = lane // heads, lax.rem(lane, heads)
    group = 128 // heads
    row = lax.broadcasted_iota(jnp.int32, (pairs, 128), 0)
    pos = base + row // heads
    same_head = lax.rem(row, heads) == lane_head
    slope = jnp.exp2((lax.axis_index("tp") * heads + lane_head + 1).astype(jnp.float32) * (-8.0 / all_heads))
    per_group = chunks // (batch // group)
    for g in range(batch // group):
        q_g = q_t[:, g * 128:(g + 1) * 128]
        scores = None
        for c in range(g * per_group, (g + 1) * per_group):
            moves(k_hbm, kbuf, k_in, c).wait()
            if c + 1 < chunks:
                moves(v_hbm, vbuf, v_in, c + 1).start()
            put_rows(kbuf, rep_k, c)
            seqs = range(c * per, (c + 1) * per)
            keys = jnp.concatenate([kbuf[b] for b in seqs], axis=1)
            query = jnp.concatenate([jnp.where(lane_seq == b - g * group, q_g, 0) for b in seqs], axis=0)
            part = jnp.dot(keys, query, preferred_element_type=jnp.float32)
            scores = part if scores is None else scores + part
            moves(kbuf, kn_hbm, k_out, c).start()
        length = jnp.zeros((1, 128), jnp.int32)
        for i in range(group):
            length = jnp.where(lane_seq == i, lens_ref[g * group + i], length)
        scores = scores * hd ** -0.5 - slope * (length - pos).astype(jnp.float32)
        valid = same_head & (pos <= length)
        scores = jnp.where(valid, scores, -1e30)
        top = jnp.max(scores, axis=0, keepdims=True)
        p = jnp.where(valid, jnp.exp(scores - top), 0.0)
        total = jnp.sum(p, axis=0, keepdims=True)
        stats = jnp.concatenate([top, total, jnp.zeros((6, 128), jnp.float32)], axis=0)
        for s in range(g * sp // (batch // group), (g + 1) * sp // (batch // group)):
            pay_ref[s, batch // sp * heads:, :] = stats
        p_t[g * 128:(g + 1) * 128, :] = p.T.astype(jnp.bfloat16)

    quad = 16 // heads
    row_seq = lax.broadcasted_iota(jnp.int32, (16, hd), 0) // heads
    for c in range(chunks):
        moves(v_hbm, vbuf, v_in, c).wait()
        put_rows(vbuf, rep_v, c)
        for b in range(c * per, (c + 1) * per, quad):
            values = jnp.concatenate([vbuf[b + i] for i in range(quad)], axis=1)
            out = jnp.dot(p_t[b * heads:b * heads + 16, :], values, preferred_element_type=jnp.float32)
            out = sum(jnp.where(row_seq == i, out[:, i * hd:(i + 1) * hd], 0.0) for i in range(quad))
            owner = b * sp // batch
            at = (b - owner * (batch // sp)) * heads
            pay_ref[owner, at:at + 16, :] = out
        moves(vbuf, vn_hbm, v_out, c).start()
    for c in range(chunks):
        moves(kbuf, kn_hbm, k_out, c).wait()
        moves(vbuf, vn_hbm, v_out, c).wait()


def attend(tp, sp, lens, x_in, gain, w_qkv, k_cache, v_cache):
    batch, slots, heads, hd = k_cache.shape
    d = x_in.shape[1]
    chunks, pieces = 8, 8
    flat = (batch, slots * heads, hd)
    vmem = pl.BlockSpec(memory_space=pltpu.VMEM)
    hbm = pl.BlockSpec(memory_space=pltpu.HBM)
    dma = pltpu.SemaphoreType.DMA
    operands = (lens, x_in, gain[None, :], w_qkv.reshape(d * 3 * heads, hd), k_cache.reshape(flat), v_cache.reshape(flat))
    pay, k_next, v_next = pl.pallas_call(
        functools.partial(attend_kernel, heads=heads, all_heads=heads * tp, sp=sp, chunks=chunks),
        out_shape=(jax.ShapeDtypeStruct((sp, batch // sp * heads + 8, hd), jnp.float32),
                   jax.ShapeDtypeStruct(flat, k_cache.dtype), jax.ShapeDtypeStruct(flat, v_cache.dtype)),
        in_specs=[hbm] * len(operands),
        out_specs=(vmem, hbm, hbm),
        scratch_shapes=[
            pltpu.SMEM(lens.shape, lens.dtype), pltpu.VMEM(x_in.shape, x_in.dtype), pltpu.VMEM((1, d), gain.dtype),
            pltpu.VMEM((d * 3 * heads, hd), jnp.bfloat16), pltpu.VMEM((d // pieces * 3 * heads, hd), jnp.float32),
            pltpu.VMEM((batch, d), jnp.bfloat16), pltpu.VMEM((3, batch * heads, hd), jnp.float32),
            pltpu.VMEM(flat, k_cache.dtype), pltpu.VMEM(flat, v_cache.dtype),
            pltpu.VMEM((batch // 2, 2, 8, hd), jnp.float32), pltpu.VMEM((batch // 2, 2, 8, hd), jnp.float32),
            pltpu.VMEM((batch * heads, slots * heads), jnp.bfloat16),
            dma((3,)), dma((pieces,)), dma((chunks,)), dma((chunks,)), dma((chunks,)), dma((chunks,)),
        ],
        compiler_params=pltpu.CompilerParams(vmem_limit_bytes=36 * 2 ** 20),
        name="attend",
    )(*(pltpu.with_memory_space_constraint(a, pltpu.HBM) for a in operands))
    return pay, k_next.reshape(k_cache.shape), v_next.reshape(v_cache.shape)


def solution(mesh):
    tp_size = mesh.shape["tp"]
    sp_size = mesh.shape["sp"]

    def local_layer(x_in, seq_lens, k_cache, v_cache, ln1_gain, w_qkv, w_out, ln2_gain, w_up, w_down):
        local_heads = k_cache.shape[2]
        head_dim = k_cache.shape[3]
        pay, k_next, v_next = attend(tp_size, sp_size, seq_lens, x_in, ln1_gain, w_qkv, k_cache, v_cache)
        x_out = tail(tp_size, sp_size, local_heads, head_dim, pay, x_in, ln2_gain, w_out, w_up, w_down)
        return x_out, k_next, v_next

    cache_spec = P("dp", "sp", "tp", None)
    in_specs = (P("dp", None), P("dp"), cache_spec, cache_spec, P(None), P(None, None, "tp", None), P("tp", None, None), P(None), P(None, "tp"), P("tp", None))
    out_specs = (P("dp", None), cache_spec, cache_spec)
    return jax.shard_map(local_layer, mesh=mesh, in_specs=in_specs, out_specs=out_specs, check_vma=False)
```

```python
import functools

import jax
import jax.numpy as jnp
from jax import lax
from jax.experimental import pallas as pl
from jax.experimental.pallas import tpu as pltpu
from jax.sharding import PartitionSpec as P

LN_EPS = 1e-5
MESH = pl.DeviceIdType.MESH


def layer_norm(x_f32, gain):
    mean = jnp.mean(x_f32, axis=-1, keepdims=True)
    centred = x_f32 - mean
    variance = jnp.mean(centred * centred, axis=-1, keepdims=True)
    return centred * lax.rsqrt(variance + LN_EPS) * gain


def gelu(x):
    return 0.5 * x * (1.0 + lax.erf(x * (0.5 ** 0.5)))


def tail_kernel(tp, sp, heads, hd, pay_ref, x_ref, gain_ref, wo_hbm, wu_hbm, wd_hbm, out_ref,
                wo, wu, wd, got_pay, att, part, got_part, r_all, h_mid, hidden, down, got_down, x_all,
                wo_sem, wu_sem, wd_sem, s1, r1, s2, r2, s3, r3, s4, r4, s5z, s5y, s5c, r5):
    my_tp = lax.axis_index("tp")
    my_sp = lax.axis_index("sp")
    rows = x_ref.shape[0] // sp
    cols = x_ref.shape[1] // tp

    barrier = pltpu.get_barrier_semaphore()
    for off in range(1, sp):
        pl.semaphore_signal(barrier, inc=1, device_id={"sp": lax.rem(my_sp + off, sp)}, device_id_type=MESH)
    for off in range(1, tp):
        pl.semaphore_signal(barrier, inc=1, device_id={"tp": lax.rem(my_tp + off, tp)}, device_id_type=MESH)

    loads = {}
    for name, src, dst, sem in (("o", wo_hbm, wo, wo_sem), ("u", wu_hbm, wu, wu_sem), ("d", wd_hbm, wd, wd_sem)):
        for j in range(tp):
            copy = pltpu.make_async_copy(src.at[:, pl.ds(j * cols, cols)], dst.at[j], sem.at[j])
            copy.start()
            loads[name, j] = copy

    pl.semaphore_wait(barrier, sp + tp - 2)

    sends = []
    for off in range(1, sp):
        peer = lax.rem(my_sp + off, sp)
        copy = pltpu.make_async_remote_copy(
            pay_ref.at[peer], got_pay.at[my_sp],
            s1.at[off], r1.at[my_sp], device_id={"sp": peer}, device_id_type=MESH)
        copy.start()
        sends.append(copy)

    def arrived(dst, sem):
        pltpu.make_async_copy(dst, dst, sem).wait()

    pairs = rows * heads
    blocks = [pay_ref[my_sp]]
    for off in range(1, sp):
        peer = lax.rem(my_sp + off, sp)
        arrived(got_pay.at[peer], r1.at[peer])
        blocks.append(got_pay[peer])
    top = functools.reduce(jnp.maximum, [b[pairs:pairs + 1] for b in blocks])
    scale = [jnp.exp(b[pairs:pairs + 1] - top) for b in blocks]
    den = sum(c * b[pairs + 1:pairs + 2] for c, b in zip(scale, blocks))
    coef = jnp.concatenate(scale + [den] * (8 - sp), axis=0).T
    coef = jnp.where(lax.rem(my_sp, 2) == 0, coef[:pairs], coef[pairs:])
    att[...] = sum(coef[:, i:i + 1] * b[:pairs] for i, b in enumerate(blocks)) / coef[:, sp:sp + 1]
    attended = jnp.concatenate([att[pl.ds(h, rows, stride=heads), :] for h in range(heads)], axis=1).astype(jnp.bfloat16)

    high = my_tp // 2
    near = (my_tp + 1 - 2 * lax.rem(my_tp, 2), 2 - high, 3 - 3 * high)
    far = near[::-1]
    split = part.shape[1]
    piece = cols // split

    def send(src, dst, send_sem, recv_sem, to):
        copy = pltpu.make_async_remote_copy(src, dst, send_sem, recv_sem, device_id=to, device_id_type=MESH)
        copy.start()
        sends.append(copy)

    def reduce_scatter(lhs, weights, buf, got, send_sem, recv_sem):
        for i in range(split):
            for peer in far:
                buf[peer, i] = jnp.dot(lhs, weights[peer, :, i * piece:(i + 1) * piece], preferred_element_type=jnp.float32)
                send(buf.at[peer, i], got.at[my_tp, i], send_sem.at[peer, i], recv_sem.at[my_tp, i], {"tp": peer})
        own = [jnp.dot(lhs, weights[my_tp, :, i * piece:(i + 1) * piece], preferred_element_type=jnp.float32)
               for i in range(split)]

        def total(i):
            out = own[i]
            for peer in near:
                arrived(got.at[peer, i], recv_sem.at[peer, i])
                out += got[peer, i]
            return out
        return total

    for j in range(tp):
        loads["o", j].wait()
    total = reduce_scatter(attended, wo, part, got_part, s2, r2)
    row0 = pl.multiple_of(my_sp * rows, rows)
    for i in range(split):
        col0 = pl.multiple_of(my_tp * cols + i * piece, piece)
        r_all[my_tp, i] = total(i) + x_ref[pl.ds(row0, rows), pl.ds(col0, piece)].astype(jnp.float32)
        for peer in far:
            send(r_all.at[my_tp, i], r_all.at[my_tp, i], s3.at[peer, i], r3.at[my_tp, i], {"tp": peer})
    for i in range(split):
        for peer in near:
            arrived(r_all.at[peer, i], r3.at[peer, i])

    r = jnp.concatenate([r_all[j, i] for j in range(tp) for i in range(split)], axis=1)
    h_mid[...] = layer_norm(r, gain_ref[...]).astype(jnp.bfloat16)

    for j in range(tp):
        loads["u", j].wait()
        up = jnp.dot(h_mid[...], wu[j], preferred_element_type=jnp.float32)
        hidden[:, j * wu.shape[2]:(j + 1) * wu.shape[2]] = gelu(up).astype(jnp.bfloat16)

    for j in range(tp):
        loads["d", j].wait()
    total = reduce_scatter(hidden[...], wd, down, got_down, s4, r4)

    side = lax.rem(my_sp + 2, sp)
    twin = my_sp + 1 - 2 * lax.rem(my_sp, 2)
    side_twin = lax.rem(twin + 2, sp)

    def pass_on(s, t, i, send_sem, to):
        send(x_all.at[s, t, i], x_all.at[s, t, i], send_sem, r5.at[s, t, i], to)

    for i in range(split):
        x_all[my_sp, my_tp, i] = (r_all[my_tp, i] + total(i)).astype(jnp.bfloat16).astype(jnp.float32)
        for peer in far:
            pass_on(my_sp, my_tp, i, s5y.at[peer, i], {"tp": peer, "sp": side})
            pass_on(my_sp, my_tp, i, s5z.at[peer, i], {"tp": peer})
        pass_on(my_sp, my_tp, i, s5y.at[my_tp, i], {"sp": side})
        pass_on(my_sp, my_tp, i, s5c.at[0, my_tp, i], {"sp": twin})
    for i in range(split):
        arrived(x_all.at[side, my_tp, i], r5.at[side, my_tp, i])
        pass_on(side, my_tp, i, s5c.at[1, my_tp, i], {"sp": twin})
        for peer in near:
            for n, who in enumerate((my_sp, side)):
                arrived(x_all.at[who, peer, i], r5.at[who, peer, i])
                pass_on(who, peer, i, s5c.at[n, peer, i], {"sp": twin})
    for who in (twin, side_twin):
        for i in range(split):
            for peer in (my_tp,) + near:
                arrived(x_all.at[who, peer, i], r5.at[who, peer, i])
    for s in range(sp):
        for t in range(tp):
            for i in range(split):
                at = t * cols + i * piece
                out_ref[s * rows:(s + 1) * rows, at:at + piece] = x_all[s, t, i].astype(jnp.bfloat16)
    for copy in sends:
        copy.wait_send()


def tail(tp, sp, heads, hd, pay, x_in, gain, w_out, w_up, w_down):
    batch, d = x_in.shape
    rows, cols = batch // sp, d // tp
    split = 1
    blocks = (tp, split, rows, cols // split)
    ff = w_up.shape[1]
    width = heads * hd
    vmem = pl.BlockSpec(memory_space=pltpu.VMEM)
    hbm = pl.BlockSpec(memory_space=pltpu.HBM)
    dma = pltpu.SemaphoreType.DMA
    return pl.pallas_call(
        functools.partial(tail_kernel, tp, sp, heads, hd),
        out_shape=jax.ShapeDtypeStruct((batch, d), jnp.bfloat16),
        in_specs=[vmem, vmem, vmem, hbm, hbm, hbm],
        out_specs=vmem,
        scratch_shapes=[
            pltpu.VMEM((tp, width, cols), jnp.bfloat16),
            pltpu.VMEM((tp, d, ff // tp), jnp.bfloat16),
            pltpu.VMEM((tp, ff, cols), jnp.bfloat16),
            pltpu.VMEM(pay.shape, jnp.float32),
            pltpu.VMEM((rows * heads, hd), jnp.float32),
            pltpu.VMEM(blocks, jnp.float32), pltpu.VMEM(blocks, jnp.float32), pltpu.VMEM(blocks, jnp.float32),
            pltpu.VMEM((rows, d), jnp.bfloat16),
            pltpu.VMEM((rows, ff), jnp.bfloat16),
            pltpu.VMEM(blocks, jnp.float32), pltpu.VMEM(blocks, jnp.float32),
            pltpu.VMEM((sp,) + blocks, jnp.float32),
            dma((tp,)), dma((tp,)), dma((tp,)),
            dma((sp,)), dma((sp,)), *[dma((tp, split))] * 8, dma((2, tp, split)), dma((sp, tp, split)),
        ],
        compiler_params=pltpu.CompilerParams(collective_id=0, has_side_effects=True, vmem_limit_bytes=24 * 2 ** 20),
        name="tail",
    )(pay, x_in, gain[None, :], *(pltpu.with_memory_space_constraint(w, pltpu.HBM) for w in (w_out.reshape(width, d), w_up, w_down)))


def attend_kernel(lens_hbm, x_hbm, gain_hbm, w_hbm, k_hbm, v_hbm, pay_ref, kn_hbm, vn_hbm,
                  lens_ref, x_ref, gain_ref, wbuf, wide, normed, qkv, kbuf, vbuf, rep_k, rep_v, p_t,
                  small_in, w_in, k_in, v_in, k_out, v_out, *, heads, all_heads, sp, chunks, ahead):
    batch, pairs, hd = kbuf.shape
    slots = pairs // heads
    per = batch // chunks
    base = lax.axis_index("sp") * slots

    def moves(src, dst, sem, c):
        part = pl.ds(c * per, per)
        return pltpu.make_async_copy(src.at[part], dst.at[part], sem.at[c])

    small = [pltpu.make_async_copy(src, dst, small_in.at[i])
             for i, (src, dst) in enumerate(((x_hbm, x_ref), (gain_hbm, gain_ref), (lens_hbm, lens_ref)))]
    for copy in small:
        copy.start()
    d = x_ref.shape[1]
    parts = 3 * heads
    depth = wide.shape[0] // parts
    pieces = d // depth
    loads = []
    for j in range(pieces):
        part = pl.ds(j * depth * parts, depth * parts)
        loads.append(pltpu.make_async_copy(w_hbm.at[part], wbuf.at[part], w_in.at[j]))
    loads += [moves(k_hbm, kbuf, k_in, c) for c in range(chunks)] + [moves(v_hbm, vbuf, v_in, c) for c in range(chunks)]
    for copy in loads[:ahead]:
        copy.start()

    def loaded(i):
        loads[i].wait()
        if i + ahead < len(loads):
            loads[i + ahead].start()

    for copy in small:
        copy.wait()
    normed[...] = layer_norm(x_ref[...].astype(jnp.float32), gain_ref[...]).astype(jnp.bfloat16)
    proj = None
    for j in range(pieces):
        loaded(j)
        wide[...] = wbuf[j * depth * parts:(j + 1) * depth * parts, :].astype(jnp.float32)
        w = jnp.concatenate([wide[pl.ds(i, depth, stride=parts), :].astype(jnp.bfloat16) for i in range(parts)], axis=1)
        part = jnp.dot(normed[:, j * depth:(j + 1) * depth], w, preferred_element_type=jnp.float32)
        proj = part if proj is None else proj + part
    for i in range(parts):
        qkv[i // heads, pl.ds(i % heads, batch, stride=heads), :] = (
            proj[:, i * hd:(i + 1) * hd].astype(jnp.bfloat16).astype(jnp.float32))

    low = lax.broadcasted_iota(jnp.int32, (1, 8, hd), 1) < heads
    for rep, i in ((rep_k, 1), (rep_v, 2)):
        new = qkv[i].reshape(batch // 2, 8, hd)
        turned = pltpu.roll(new, heads, 1)
        rep[:, 0] = jnp.where(low, new, turned)
        rep[:, 1] = jnp.where(low, turned, new)

    row_slot = lax.broadcasted_iota(jnp.int32, (16, hd), 0) // heads

    def put_rows(buf, rep, c):
        for b in range(c * per, (c + 1) * per):
            slot = lens_ref[b] - base

            @pl.when((slot >= 0) & (slot < slots))
            def _():
                span = pl.ds(pl.multiple_of(slot // 4 * 16, 16), 16)
                old = buf[b, span, :].astype(jnp.float32)
                new = jnp.concatenate([rep[b // 2, b % 2]] * 2, axis=0)
                buf[b, span, :] = jnp.where(row_slot == lax.rem(slot, 4), new, old).astype(buf.dtype)

    q_t = qkv[0].T.astype(jnp.bfloat16)
    lane = lax.broadcasted_iota(jnp.int32, (1, 128), 1)
    lane_seq, lane_head = lane // heads, lax.rem(lane, heads)
    group = 128 // heads
    row = lax.broadcasted_iota(jnp.int32, (pairs, 128), 0)
    pos = base + row // heads
    same_head = lax.rem(row, heads) == lane_head
    slope = jnp.exp2((lax.axis_index("tp") * heads + lane_head + 1).astype(jnp.float32) * (-8.0 / all_heads))
    per_group = chunks // (batch // group)
    for g in range(batch // group):
        q_g = q_t[:, g * 128:(g + 1) * 128]
        scores = None
        for c in range(g * per_group, (g + 1) * per_group):
            loaded(pieces + c)
            put_rows(kbuf, rep_k, c)
            seqs = range(c * per, (c + 1) * per)
            keys = jnp.concatenate([kbuf[b] for b in seqs], axis=1)
            query = jnp.concatenate([jnp.where(lane_seq == b - g * group, q_g, 0) for b in seqs], axis=0)
            part = jnp.dot(keys, query, preferred_element_type=jnp.float32)
            scores = part if scores is None else scores + part
            moves(kbuf, kn_hbm, k_out, c).start()
        length = jnp.zeros((1, 128), jnp.int32)
        for i in range(group):
            length = jnp.where(lane_seq == i, lens_ref[g * group + i], length)
        scores = scores * hd ** -0.5 - slope * (length - pos).astype(jnp.float32)
        valid = same_head & (pos <= length)
        scores = jnp.where(valid, scores, -1e30)
        top = jnp.max(scores, axis=0, keepdims=True)
        p = jnp.where(valid, jnp.exp(scores - top), 0.0)
        total = jnp.sum(p, axis=0, keepdims=True)
        stats = jnp.concatenate([top, total, jnp.zeros((6, 128), jnp.float32)], axis=0)
        for s in range(g * sp // (batch // group), (g + 1) * sp // (batch // group)):
            pay_ref[s, batch // sp * heads:, :] = stats
        p_t[g * 128:(g + 1) * 128, :] = p.T.astype(jnp.bfloat16)

    quad = 16 // heads
    row_seq = lax.broadcasted_iota(jnp.int32, (16, hd), 0) // heads
    for c in range(chunks):
        loaded(pieces + chunks + c)
        put_rows(vbuf, rep_v, c)
        for b in range(c * per, (c + 1) * per, quad):
            values = jnp.concatenate([vbuf[b + i] for i in range(quad)], axis=1)
            out = jnp.dot(p_t[b * heads:b * heads + 16, :], values, preferred_element_type=jnp.float32)
            out = sum(jnp.where(row_seq == i, out[:, i * hd:(i + 1) * hd], 0.0) for i in range(quad))
            owner = b * sp // batch
            at = (b - owner * (batch // sp)) * heads
            pay_ref[owner, at:at + 16, :] = out
        moves(vbuf, vn_hbm, v_out, c).start()
    for c in range(chunks):
        moves(kbuf, kn_hbm, k_out, c).wait()
        moves(vbuf, vn_hbm, v_out, c).wait()


def attend(tp, sp, lens, x_in, gain, w_qkv, k_cache, v_cache):
    batch, slots, heads, hd = k_cache.shape
    d = x_in.shape[1]
    chunks, pieces, ahead = 4, 4, 4
    flat = (batch, slots * heads, hd)
    vmem = pl.BlockSpec(memory_space=pltpu.VMEM)
    hbm = pl.BlockSpec(memory_space=pltpu.HBM)
    dma = pltpu.SemaphoreType.DMA
    operands = (lens, x_in, gain[None, :], w_qkv.reshape(d * 3 * heads, hd), k_cache.reshape(flat), v_cache.reshape(flat))
    pay, k_next, v_next = pl.pallas_call(
        functools.partial(attend_kernel, heads=heads, all_heads=heads * tp, sp=sp, chunks=chunks, ahead=ahead),
        out_shape=(jax.ShapeDtypeStruct((sp, batch // sp * heads + 8, hd), jnp.float32),
                   jax.ShapeDtypeStruct(flat, k_cache.dtype), jax.ShapeDtypeStruct(flat, v_cache.dtype)),
        in_specs=[hbm] * len(operands),
        out_specs=(vmem, hbm, hbm),
        scratch_shapes=[
            pltpu.SMEM(lens.shape, lens.dtype), pltpu.VMEM(x_in.shape, x_in.dtype), pltpu.VMEM((1, d), gain.dtype),
            pltpu.VMEM((d * 3 * heads, hd), jnp.bfloat16), pltpu.VMEM((d // pieces * 3 * heads, hd), jnp.float32),
            pltpu.VMEM((batch, d), jnp.bfloat16), pltpu.VMEM((3, batch * heads, hd), jnp.float32),
            pltpu.VMEM(flat, k_cache.dtype), pltpu.VMEM(flat, v_cache.dtype),
            pltpu.VMEM((batch // 2, 2, 8, hd), jnp.float32), pltpu.VMEM((batch // 2, 2, 8, hd), jnp.float32),
            pltpu.VMEM((batch * heads, slots * heads), jnp.bfloat16),
            dma((3,)), dma((pieces,)), dma((chunks,)), dma((chunks,)), dma((chunks,)), dma((chunks,)),
        ],
        compiler_params=pltpu.CompilerParams(vmem_limit_bytes=36 * 2 ** 20),
        name="attend",
    )(*(pltpu.with_memory_space_constraint(a, pltpu.HBM) for a in operands))
    return pay, k_next.reshape(k_cache.shape), v_next.reshape(v_cache.shape)


def solution(mesh):
    tp_size = mesh.shape["tp"]
    sp_size = mesh.shape["sp"]

    def local_layer(x_in, seq_lens, k_cache, v_cache, ln1_gain, w_qkv, w_out, ln2_gain, w_up, w_down):
        local_heads = k_cache.shape[2]
        head_dim = k_cache.shape[3]
        pay, k_next, v_next = attend(tp_size, sp_size, seq_lens, x_in, ln1_gain, w_qkv, k_cache, v_cache)
        x_out = tail(tp_size, sp_size, local_heads, head_dim, pay, x_in, ln2_gain, w_out, w_up, w_down)
        return x_out, k_next, v_next

    cache_spec = P("dp", "sp", "tp", None)
    in_specs = (P("dp", None), P("dp"), cache_spec, cache_spec, P(None), P(None, None, "tp", None), P("tp", None, None), P(None), P(None, "tp"), P("tp", None))
    out_specs = (P("dp", None), cache_spec, cache_spec)
    return jax.shard_map(local_layer, mesh=mesh, in_specs=in_specs, out_specs=out_specs, check_vma=False)
```

```python
import functools

import jax
import jax.numpy as jnp
from jax import lax
from jax.experimental import pallas as pl
from jax.experimental.pallas import tpu as pltpu
from jax.sharding import PartitionSpec as P

LN_EPS = 1e-5
MESH = pl.DeviceIdType.MESH


def layer_norm(x_f32, gain):
    mean = jnp.mean(x_f32, axis=-1, keepdims=True)
    centred = x_f32 - mean
    variance = jnp.mean(centred * centred, axis=-1, keepdims=True)
    return centred * lax.rsqrt(variance + LN_EPS) * gain


def gelu(x):
    return 0.5 * x * (1.0 + lax.erf(x * (0.5 ** 0.5)))


def tail_kernel(tp, sp, heads, hd, stats_ref, p_ref, v_ref, x_ref, gain_ref, wo_hbm, wu_hbm, wd_hbm, out_ref,
                wo, wu, wd, pay, got_pay, att, part, got_part, r_all, h_mid, hidden, down, got_down, x_all,
                wo_sem, wu_sem, wd_sem, s1, r1, s2, r2, s3, r3, s4, r4, s5z, s5y, s5c, r5):
    my_tp = lax.axis_index("tp")
    my_sp = lax.axis_index("sp")
    rows = x_ref.shape[0] // sp
    cols = x_ref.shape[1] // tp

    barrier = pltpu.get_barrier_semaphore()
    for off in range(1, sp):
        pl.semaphore_signal(barrier, inc=1, device_id={"sp": lax.rem(my_sp + off, sp)}, device_id_type=MESH)
    for off in range(1, tp):
        pl.semaphore_signal(barrier, inc=1, device_id={"tp": lax.rem(my_tp + off, tp)}, device_id_type=MESH)

    loads = {}
    for name, src, dst, sem in (("o", wo_hbm, wo, wo_sem), ("u", wu_hbm, wu, wu_sem), ("d", wd_hbm, wd, wd_sem)):
        for j in range(tp):
            copy = pltpu.make_async_copy(src.at[:, pl.ds(j * cols, cols)], dst.at[j], sem.at[j])
            copy.start()
            loads[name, j] = copy

    sends = []
    side = lax.rem(my_sp + 2, sp)
    twin = my_sp + 1 - 2 * lax.rem(my_sp, 2)
    side_twin = lax.rem(twin + 2, sp)
    order = [side, side_twin, twin, my_sp]
    quad = 16 // heads
    row_seq = lax.broadcasted_iota(jnp.int32, (16, hd), 0) // heads
    for n, owner in enumerate(order):
        for i in range(0, rows, quad):
            first = owner * rows + i
            weights = p_ref[pl.ds(pl.multiple_of(first * heads, 16), 16), :]
            values = jnp.concatenate([v_ref[first + m] for m in range(quad)], axis=1)
            out = jnp.dot(weights, values, preferred_element_type=jnp.float32)
            pay[owner, i * heads:i * heads + 16, :] = sum(
                jnp.where(row_seq == m, out[:, m * hd:(m + 1) * hd], 0.0) for m in range(quad))
        pay[owner, rows * heads:, :] = stats_ref[owner]
        if n == 0:
            pl.semaphore_wait(barrier, sp + tp - 2)
        if n < sp - 1:
            copy = pltpu.make_async_remote_copy(pay.at[owner], got_pay.at[my_sp], s1.at[owner], r1.at[my_sp],
                                                device_id={"sp": owner}, device_id_type=MESH)
            copy.start()
            sends.append(copy)

    def arrived(dst, sem):
        pltpu.make_async_copy(dst, dst, sem).wait()

    pairs = rows * heads
    blocks = [pay[my_sp]]
    for off in range(1, sp):
        peer = lax.rem(my_sp + off, sp)
        arrived(got_pay.at[peer], r1.at[peer])
        blocks.append(got_pay[peer])
    top = functools.reduce(jnp.maximum, [b[pairs:pairs + 1] for b in blocks])
    scale = [jnp.exp(b[pairs:pairs + 1] - top) for b in blocks]
    den = sum(c * b[pairs + 1:pairs + 2] for c, b in zip(scale, blocks))
    coef = jnp.concatenate(scale + [den] * (8 - sp), axis=0).T
    coef = jnp.where(lax.rem(my_sp, 2) == 0, coef[:pairs], coef[pairs:])
    att[...] = sum(coef[:, i:i + 1] * b[:pairs] for i, b in enumerate(blocks)) / coef[:, sp:sp + 1]
    attended = jnp.concatenate([att[pl.ds(h, rows, stride=heads), :] for h in range(heads)], axis=1).astype(jnp.bfloat16)

    high = my_tp // 2
    near = (my_tp + 1 - 2 * lax.rem(my_tp, 2), 2 - high, 3 - 3 * high)
    far = near[::-1]
    split = part.shape[1]
    piece = cols // split

    def send(src, dst, send_sem, recv_sem, to):
        copy = pltpu.make_async_remote_copy(src, dst, send_sem, recv_sem, device_id=to, device_id_type=MESH)
        copy.start()
        sends.append(copy)

    def reduce_scatter(lhs, weights, buf, got, send_sem, recv_sem):
        for i in range(split):
            for peer in far:
                buf[peer, i] = jnp.dot(lhs, weights[peer, :, i * piece:(i + 1) * piece], preferred_element_type=jnp.float32)
                send(buf.at[peer, i], got.at[my_tp, i], send_sem.at[peer, i], recv_sem.at[my_tp, i], {"tp": peer})
        own = [jnp.dot(lhs, weights[my_tp, :, i * piece:(i + 1) * piece], preferred_element_type=jnp.float32)
               for i in range(split)]

        def total(i):
            out = own[i]
            for peer in near:
                arrived(got.at[peer, i], recv_sem.at[peer, i])
                out += got[peer, i]
            return out
        return total

    for j in range(tp):
        loads["o", j].wait()
    total = reduce_scatter(attended, wo, part, got_part, s2, r2)
    row0 = pl.multiple_of(my_sp * rows, rows)
    for i in range(split):
        col0 = pl.multiple_of(my_tp * cols + i * piece, piece)
        r_all[my_tp, i] = total(i) + x_ref[pl.ds(row0, rows), pl.ds(col0, piece)].astype(jnp.float32)
        for peer in far:
            send(r_all.at[my_tp, i], r_all.at[my_tp, i], s3.at[peer, i], r3.at[my_tp, i], {"tp": peer})
    for i in range(split):
        for peer in near:
            arrived(r_all.at[peer, i], r3.at[peer, i])

    r = jnp.concatenate([r_all[j, i] for j in range(tp) for i in range(split)], axis=1)
    h_mid[...] = layer_norm(r, gain_ref[...]).astype(jnp.bfloat16)

    for j in range(tp):
        loads["u", j].wait()
        up = jnp.dot(h_mid[...], wu[j], preferred_element_type=jnp.float32)
        hidden[:, j * wu.shape[2]:(j + 1) * wu.shape[2]] = gelu(up).astype(jnp.bfloat16)

    for j in range(tp):
        loads["d", j].wait()
    total = reduce_scatter(hidden[...], wd, down, got_down, s4, r4)

    def pass_on(s, t, i, send_sem, to):
        send(x_all.at[s, t, i], x_all.at[s, t, i], send_sem, r5.at[s, t, i], to)

    for i in range(split):
        x_all[my_sp, my_tp, i] = (r_all[my_tp, i] + total(i)).astype(jnp.bfloat16).astype(jnp.float32)
        for peer in far:
            pass_on(my_sp, my_tp, i, s5y.at[peer, i], {"tp": peer, "sp": side})
            pass_on(my_sp, my_tp, i, s5z.at[peer, i], {"tp": peer})
        pass_on(my_sp, my_tp, i, s5y.at[my_tp, i], {"sp": side})
        pass_on(my_sp, my_tp, i, s5c.at[0, my_tp, i], {"sp": twin})
    for i in range(split):
        arrived(x_all.at[side, my_tp, i], r5.at[side, my_tp, i])
        pass_on(side, my_tp, i, s5c.at[1, my_tp, i], {"sp": twin})
        for peer in near:
            for n, who in enumerate((my_sp, side)):
                arrived(x_all.at[who, peer, i], r5.at[who, peer, i])
                pass_on(who, peer, i, s5c.at[n, peer, i], {"sp": twin})
    for who in (twin, side_twin):
        for i in range(split):
            for peer in (my_tp,) + near:
                arrived(x_all.at[who, peer, i], r5.at[who, peer, i])
    for s in range(sp):
        for t in range(tp):
            for i in range(split):
                at = t * cols + i * piece
                out_ref[s * rows:(s + 1) * rows, at:at + piece] = x_all[s, t, i].astype(jnp.bfloat16)
    for copy in sends:
        copy.wait_send()


def tail(tp, sp, heads, hd, stats, p, v, x_in, gain, w_out, w_up, w_down):
    batch, d = x_in.shape
    rows, cols = batch // sp, d // tp
    split = 1
    blocks = (tp, split, rows, cols // split)
    ff = w_up.shape[1]
    width = heads * hd
    pay = (sp, rows * heads + 8, hd)
    vmem = pl.BlockSpec(memory_space=pltpu.VMEM)
    hbm = pl.BlockSpec(memory_space=pltpu.HBM)
    dma = pltpu.SemaphoreType.DMA
    return pl.pallas_call(
        functools.partial(tail_kernel, tp, sp, heads, hd),
        out_shape=jax.ShapeDtypeStruct((batch, d), jnp.bfloat16),
        in_specs=[vmem] * 5 + [hbm] * 3,
        out_specs=vmem,
        scratch_shapes=[
            pltpu.VMEM((tp, width, cols), jnp.bfloat16),
            pltpu.VMEM((tp, d, ff // tp), jnp.bfloat16),
            pltpu.VMEM((tp, ff, cols), jnp.bfloat16),
            pltpu.VMEM(pay, jnp.float32), pltpu.VMEM(pay, jnp.float32),
            pltpu.VMEM((rows * heads, hd), jnp.float32),
            pltpu.VMEM(blocks, jnp.float32), pltpu.VMEM(blocks, jnp.float32), pltpu.VMEM(blocks, jnp.float32),
            pltpu.VMEM((rows, d), jnp.bfloat16),
            pltpu.VMEM((rows, ff), jnp.bfloat16),
            pltpu.VMEM(blocks, jnp.float32), pltpu.VMEM(blocks, jnp.float32),
            pltpu.VMEM((sp,) + blocks, jnp.float32),
            dma((tp,)), dma((tp,)), dma((tp,)),
            dma((sp,)), dma((sp,)), *[dma((tp, split))] * 8, dma((2, tp, split)), dma((sp, tp, split)),
        ],
        compiler_params=pltpu.CompilerParams(collective_id=0, has_side_effects=True, vmem_limit_bytes=24 * 2 ** 20),
        name="tail",
    )(stats, p, v, x_in, gain[None, :], *(pltpu.with_memory_space_constraint(w, pltpu.HBM) for w in (w_out.reshape(width, d), w_up, w_down)))


def attend_kernel(lens_hbm, x_hbm, gain_hbm, w_hbm, k_hbm, v_hbm, stats_ref, p_t, vbuf, kn_hbm, vn_hbm,
                  lens_ref, x_ref, gain_ref, wbuf, wide, normed, qkv, kbuf, rep_k, rep_v,
                  small_in, w_in, k_in, v_in, k_out, v_out, *, heads, all_heads, sp, chunks, ahead):
    batch, pairs, hd = kbuf.shape
    slots = pairs // heads
    per = batch // chunks
    base = lax.axis_index("sp") * slots

    def moves(src, dst, sem, c):
        part = pl.ds(c * per, per)
        return pltpu.make_async_copy(src.at[part], dst.at[part], sem.at[c])

    small = [pltpu.make_async_copy(src, dst, small_in.at[i])
             for i, (src, dst) in enumerate(((x_hbm, x_ref), (gain_hbm, gain_ref), (lens_hbm, lens_ref)))]
    for copy in small:
        copy.start()
    d = x_ref.shape[1]
    parts = 3 * heads
    depth = wide.shape[0] // parts
    pieces = d // depth
    loads = []
    for j in range(pieces):
        part = pl.ds(j * depth * parts, depth * parts)
        loads.append(pltpu.make_async_copy(w_hbm.at[part], wbuf.at[part], w_in.at[j]))
    loads += [moves(k_hbm, kbuf, k_in, c) for c in range(chunks)] + [moves(v_hbm, vbuf, v_in, c) for c in range(chunks)]
    for copy in loads[:ahead]:
        copy.start()

    def loaded(i):
        loads[i].wait()
        if i + ahead < len(loads):
            loads[i + ahead].start()

    for copy in small:
        copy.wait()
    normed[...] = layer_norm(x_ref[...].astype(jnp.float32), gain_ref[...]).astype(jnp.bfloat16)
    proj = None
    for j in range(pieces):
        loaded(j)
        wide[...] = wbuf[j * depth * parts:(j + 1) * depth * parts, :].astype(jnp.float32)
        w = jnp.concatenate([wide[pl.ds(i, depth, stride=parts), :].astype(jnp.bfloat16) for i in range(parts)], axis=1)
        part = jnp.dot(normed[:, j * depth:(j + 1) * depth], w, preferred_element_type=jnp.float32)
        proj = part if proj is None else proj + part
    for i in range(parts):
        qkv[i // heads, pl.ds(i % heads, batch, stride=heads), :] = (
            proj[:, i * hd:(i + 1) * hd].astype(jnp.bfloat16).astype(jnp.float32))

    low = lax.broadcasted_iota(jnp.int32, (1, 8, hd), 1) < heads
    for rep, i in ((rep_k, 1), (rep_v, 2)):
        new = qkv[i].reshape(batch // 2, 8, hd)
        turned = pltpu.roll(new, heads, 1)
        rep[:, 0] = jnp.where(low, new, turned)
        rep[:, 1] = jnp.where(low, turned, new)

    row_slot = lax.broadcasted_iota(jnp.int32, (16, hd), 0) // heads

    def put_rows(buf, rep, c):
        for b in range(c * per, (c + 1) * per):
            slot = lens_ref[b] - base

            @pl.when((slot >= 0) & (slot < slots))
            def _():
                span = pl.ds(pl.multiple_of(slot // 4 * 16, 16), 16)
                old = buf[b, span, :].astype(jnp.float32)
                new = jnp.concatenate([rep[b // 2, b % 2]] * 2, axis=0)
                buf[b, span, :] = jnp.where(row_slot == lax.rem(slot, 4), new, old).astype(buf.dtype)

    def store_v(c):
        loaded(pieces + chunks + c)
        put_rows(vbuf, rep_v, c)
        moves(vbuf, vn_hbm, v_out, c).start()

    q_t = qkv[0].T.astype(jnp.bfloat16)
    lane = lax.broadcasted_iota(jnp.int32, (1, 128), 1)
    lane_seq, lane_head = lane // heads, lax.rem(lane, heads)
    group = 128 // heads
    row = lax.broadcasted_iota(jnp.int32, (pairs, 128), 0)
    pos = base + row // heads
    same_head = lax.rem(row, heads) == lane_head
    slope = jnp.exp2((lax.axis_index("tp") * heads + lane_head + 1).astype(jnp.float32) * (-8.0 / all_heads))
    per_group = chunks // (batch // group)
    for g in range(batch // group):
        q_g = q_t[:, g * 128:(g + 1) * 128]
        scores = None
        for c in range(g * per_group, (g + 1) * per_group):
            loaded(pieces + c)
            put_rows(kbuf, rep_k, c)
            seqs = range(c * per, (c + 1) * per)
            keys = jnp.concatenate([kbuf[b] for b in seqs], axis=1)
            query = jnp.concatenate([jnp.where(lane_seq == b - g * group, q_g, 0) for b in seqs], axis=0)
            part = jnp.dot(keys, query, preferred_element_type=jnp.float32)
            scores = part if scores is None else scores + part
            moves(kbuf, kn_hbm, k_out, c).start()
            if c >= 1:
                store_v(c - 1)
        length = jnp.zeros((1, 128), jnp.int32)
        for i in range(group):
            length = jnp.where(lane_seq == i, lens_ref[g * group + i], length)
        scores = scores * hd ** -0.5 - slope * (length - pos).astype(jnp.float32)
        valid = same_head & (pos <= length)
        scores = jnp.where(valid, scores, -1e30)
        top = jnp.max(scores, axis=0, keepdims=True)
        p = jnp.where(valid, jnp.exp(scores - top), 0.0)
        total = jnp.sum(p, axis=0, keepdims=True)
        stats = jnp.concatenate([top, total, jnp.zeros((6, 128), jnp.float32)], axis=0)
        for s in range(g * sp // (batch // group), (g + 1) * sp // (batch // group)):
            stats_ref[s] = stats
        p_t[g * 128:(g + 1) * 128, :] = p.T.astype(jnp.bfloat16)

    for c in range(chunks - 1, chunks):
        store_v(c)
    for c in range(chunks):
        moves(kbuf, kn_hbm, k_out, c).wait()
        moves(vbuf, vn_hbm, v_out, c).wait()


def attend(tp, sp, lens, x_in, gain, w_qkv, k_cache, v_cache):
    batch, slots, heads, hd = k_cache.shape
    d = x_in.shape[1]
    chunks, pieces, ahead = 4, 4, 5
    flat = (batch, slots * heads, hd)
    vmem = pl.BlockSpec(memory_space=pltpu.VMEM)
    hbm = pl.BlockSpec(memory_space=pltpu.HBM)
    dma = pltpu.SemaphoreType.DMA
    operands = (lens, x_in, gain[None, :], w_qkv.reshape(d * 3 * heads, hd), k_cache.reshape(flat), v_cache.reshape(flat))
    return pl.pallas_call(
        functools.partial(attend_kernel, heads=heads, all_heads=heads * tp, sp=sp, chunks=chunks, ahead=ahead),
        out_shape=(pltpu.VMEM((sp, 8, hd), jnp.float32), pltpu.VMEM((batch * heads, slots * heads), jnp.bfloat16),
                   pltpu.VMEM(flat, v_cache.dtype),
                   jax.ShapeDtypeStruct(flat, k_cache.dtype), jax.ShapeDtypeStruct(flat, v_cache.dtype)),
        in_specs=[hbm] * len(operands),
        out_specs=(vmem, vmem, vmem, hbm, hbm),
        scratch_shapes=[
            pltpu.SMEM(lens.shape, lens.dtype), pltpu.VMEM(x_in.shape, x_in.dtype), pltpu.VMEM((1, d), gain.dtype),
            pltpu.VMEM((d * 3 * heads, hd), jnp.bfloat16), pltpu.VMEM((d // pieces * 3 * heads, hd), jnp.float32),
            pltpu.VMEM((batch, d), jnp.bfloat16), pltpu.VMEM((3, batch * heads, hd), jnp.float32),
            pltpu.VMEM(flat, k_cache.dtype),
            pltpu.VMEM((batch // 2, 2, 8, hd), jnp.float32), pltpu.VMEM((batch // 2, 2, 8, hd), jnp.float32),
            dma((3,)), dma((pieces,)), dma((chunks,)), dma((chunks,)), dma((chunks,)), dma((chunks,)),
        ],
        compiler_params=pltpu.CompilerParams(vmem_limit_bytes=36 * 2 ** 20),
        name="attend",
    )(*(pltpu.with_memory_space_constraint(a, pltpu.HBM) for a in operands))


def solution(mesh):
    tp_size = mesh.shape["tp"]
    sp_size = mesh.shape["sp"]

    def local_layer(x_in, seq_lens, k_cache, v_cache, ln1_gain, w_qkv, w_out, ln2_gain, w_up, w_down):
        local_heads = k_cache.shape[2]
        head_dim = k_cache.shape[3]
        stats, p, v, k_next, v_next = attend(tp_size, sp_size, seq_lens, x_in, ln1_gain, w_qkv, k_cache, v_cache)
        x_out = tail(tp_size, sp_size, local_heads, head_dim, stats, p, v, x_in, ln2_gain, w_out, w_up, w_down)
        return x_out, k_next.reshape(k_cache.shape), v_next.reshape(v_cache.shape)

    cache_spec = P("dp", "sp", "tp", None)
    in_specs = (P("dp", None), P("dp"), cache_spec, cache_spec, P(None), P(None, None, "tp", None), P("tp", None, None), P(None), P(None, "tp"), P("tp", None))
    out_specs = (P("dp", None), cache_spec, cache_spec)
    return jax.shard_map(local_layer, mesh=mesh, in_specs=in_specs, out_specs=out_specs, check_vma=False)
```

```python
import functools

import jax
import jax.numpy as jnp
from jax import lax
from jax.experimental import pallas as pl
from jax.experimental.pallas import tpu as pltpu
from jax.sharding import PartitionSpec as P

LN_EPS = 1e-5
MESH = pl.DeviceIdType.MESH


def layer_norm(x_f32, gain):
    mean = jnp.mean(x_f32, axis=-1, keepdims=True)
    centred = x_f32 - mean
    variance = jnp.mean(centred * centred, axis=-1, keepdims=True)
    return centred * lax.rsqrt(variance + LN_EPS) * gain


def gelu(x):
    return 0.5 * x * (1.0 + lax.erf(x * (0.5 ** 0.5)))


def tail_kernel(tp, sp, heads, hd, pay_ref, x_ref, gain_ref, wo_hbm, wu_hbm, wd_hbm, out_ref,
                wo, wu, wd, got_pay, att, part, got_part, r_all, h_mid, hidden, down, got_down, x_all,
                wo_sem, wu_sem, wd_sem, s1, r1, s2, r2, s3, r3, s4, r4, s5z, s5y, s5c, r5):
    my_tp = lax.axis_index("tp")
    my_sp = lax.axis_index("sp")
    rows = x_ref.shape[0] // sp
    cols = x_ref.shape[1] // tp

    barrier = pltpu.get_barrier_semaphore()
    for off in range(1, sp):
        pl.semaphore_signal(barrier, inc=1, device_id={"sp": lax.rem(my_sp + off, sp)}, device_id_type=MESH)
    for off in range(1, tp):
        pl.semaphore_signal(barrier, inc=1, device_id={"tp": lax.rem(my_tp + off, tp)}, device_id_type=MESH)

    loads = {}
    for name, src, dst, sem in (("o", wo_hbm, wo, wo_sem), ("u", wu_hbm, wu, wu_sem), ("d", wd_hbm, wd, wd_sem)):
        for j in range(tp):
            copy = pltpu.make_async_copy(src.at[:, pl.ds(j * cols, cols)], dst.at[j], sem.at[j])
            copy.start()
            loads[name, j] = copy

    pl.semaphore_wait(barrier, sp + tp - 2)

    side = lax.rem(my_sp + 2, sp)
    twin = my_sp + 1 - 2 * lax.rem(my_sp, 2)
    side_twin = lax.rem(twin + 2, sp)
    sends = []
    for off, peer in enumerate((side, side_twin, twin)):
        copy = pltpu.make_async_remote_copy(
            pay_ref.at[peer], got_pay.at[my_sp],
            s1.at[off], r1.at[my_sp], device_id={"sp": peer}, device_id_type=MESH)
        copy.start()
        sends.append(copy)

    def arrived(dst, sem):
        pltpu.make_async_copy(dst, dst, sem).wait()

    pairs = rows * heads
    blocks = [pay_ref[my_sp]]
    for off in range(1, sp):
        peer = lax.rem(my_sp + off, sp)
        arrived(got_pay.at[peer], r1.at[peer])
        blocks.append(got_pay[peer])
    top = functools.reduce(jnp.maximum, [b[pairs:pairs + 1] for b in blocks])
    scale = [jnp.exp(b[pairs:pairs + 1] - top) for b in blocks]
    den = sum(c * b[pairs + 1:pairs + 2] for c, b in zip(scale, blocks))
    coef = jnp.concatenate(scale + [den] * (8 - sp), axis=0).T
    coef = jnp.where(lax.rem(my_sp, 2) == 0, coef[:pairs], coef[pairs:])
    att[...] = sum(coef[:, i:i + 1] * b[:pairs] for i, b in enumerate(blocks)) / coef[:, sp:sp + 1]
    attended = jnp.concatenate([att[pl.ds(h, rows, stride=heads), :] for h in range(heads)], axis=1).astype(jnp.bfloat16)

    high = my_tp // 2
    near = (my_tp + 1 - 2 * lax.rem(my_tp, 2), 2 - high, 3 - 3 * high)
    far = near[::-1]
    split = part.shape[1]
    piece = cols // split

    def send(src, dst, send_sem, recv_sem, to):
        copy = pltpu.make_async_remote_copy(src, dst, send_sem, recv_sem, device_id=to, device_id_type=MESH)
        copy.start()
        sends.append(copy)

    def reduce_scatter(lhs, weights, buf, got, send_sem, recv_sem):
        for i in range(split):
            for peer in far:
                buf[peer, i] = jnp.dot(lhs, weights[peer, :, i * piece:(i + 1) * piece], preferred_element_type=jnp.float32)
                send(buf.at[peer, i], got.at[my_tp, i], send_sem.at[peer, i], recv_sem.at[my_tp, i], {"tp": peer})
        own = [jnp.dot(lhs, weights[my_tp, :, i * piece:(i + 1) * piece], preferred_element_type=jnp.float32)
               for i in range(split)]

        def total(i):
            out = own[i]
            for peer in near:
                arrived(got.at[peer, i], recv_sem.at[peer, i])
                out += got[peer, i]
            return out
        return total

    for j in range(tp):
        loads["o", j].wait()
    total = reduce_scatter(attended, wo, part, got_part, s2, r2)
    row0 = pl.multiple_of(my_sp * rows, rows)
    for i in range(split):
        col0 = pl.multiple_of(my_tp * cols + i * piece, piece)
        r_all[my_tp, i] = total(i) + x_ref[pl.ds(row0, rows), pl.ds(col0, piece)].astype(jnp.float32)
        for peer in far:
            send(r_all.at[my_tp, i], r_all.at[my_tp, i], s3.at[peer, i], r3.at[my_tp, i], {"tp": peer})
    for i in range(split):
        for peer in near:
            arrived(r_all.at[peer, i], r3.at[peer, i])

    r = jnp.concatenate([r_all[j, i] for j in range(tp) for i in range(split)], axis=1)
    h_mid[...] = layer_norm(r, gain_ref[...]).astype(jnp.bfloat16)

    for j in range(tp):
        loads["u", j].wait()
        up = jnp.dot(h_mid[...], wu[j], preferred_element_type=jnp.float32)
        hidden[:, j * wu.shape[2]:(j + 1) * wu.shape[2]] = gelu(up).astype(jnp.bfloat16)

    for j in range(tp):
        loads["d", j].wait()
    total = reduce_scatter(hidden[...], wd, down, got_down, s4, r4)


    def pass_on(s, t, i, send_sem, to):
        send(x_all.at[s, t, i], x_all.at[s, t, i], send_sem, r5.at[s, t, i], to)

    for i in range(split):
        x_all[my_sp, my_tp, i] = (r_all[my_tp, i] + total(i)).astype(jnp.bfloat16).astype(jnp.float32)
        for peer in far:
            pass_on(my_sp, my_tp, i, s5y.at[peer, i], {"tp": peer, "sp": side})
            pass_on(my_sp, my_tp, i, s5z.at[peer, i], {"tp": peer})
        pass_on(my_sp, my_tp, i, s5y.at[my_tp, i], {"sp": side})
        pass_on(my_sp, my_tp, i, s5c.at[0, my_tp, i], {"sp": twin})
    for i in range(split):
        arrived(x_all.at[side, my_tp, i], r5.at[side, my_tp, i])
        pass_on(side, my_tp, i, s5c.at[1, my_tp, i], {"sp": twin})
        for peer in near:
            for n, who in enumerate((my_sp, side)):
                arrived(x_all.at[who, peer, i], r5.at[who, peer, i])
                pass_on(who, peer, i, s5c.at[n, peer, i], {"sp": twin})
    for who in (twin, side_twin):
        for i in range(split):
            for peer in (my_tp,) + near:
                arrived(x_all.at[who, peer, i], r5.at[who, peer, i])
    for s in range(sp):
        for t in range(tp):
            for i in range(split):
                at = t * cols + i * piece
                out_ref[s * rows:(s + 1) * rows, at:at + piece] = x_all[s, t, i].astype(jnp.bfloat16)
    for copy in sends:
        copy.wait_send()


def tail(tp, sp, heads, hd, pay, x_in, gain, w_out, w_up, w_down):
    batch, d = x_in.shape
    rows, cols = batch // sp, d // tp
    split = 1
    blocks = (tp, split, rows, cols // split)
    ff = w_up.shape[1]
    width = heads * hd
    vmem = pl.BlockSpec(memory_space=pltpu.VMEM)
    hbm = pl.BlockSpec(memory_space=pltpu.HBM)
    dma = pltpu.SemaphoreType.DMA
    return pl.pallas_call(
        functools.partial(tail_kernel, tp, sp, heads, hd),
        out_shape=jax.ShapeDtypeStruct((batch, d), jnp.bfloat16),
        in_specs=[vmem, vmem, vmem, hbm, hbm, hbm],
        out_specs=vmem,
        scratch_shapes=[
            pltpu.VMEM((tp, width, cols), jnp.bfloat16),
            pltpu.VMEM((tp, d, ff // tp), jnp.bfloat16),
            pltpu.VMEM((tp, ff, cols), jnp.bfloat16),
            pltpu.VMEM(pay.shape, jnp.float32),
            pltpu.VMEM((rows * heads, hd), jnp.float32),
            pltpu.VMEM(blocks, jnp.float32), pltpu.VMEM(blocks, jnp.float32), pltpu.VMEM(blocks, jnp.float32),
            pltpu.VMEM((rows, d), jnp.bfloat16),
            pltpu.VMEM((rows, ff), jnp.bfloat16),
            pltpu.VMEM(blocks, jnp.float32), pltpu.VMEM(blocks, jnp.float32),
            pltpu.VMEM((sp,) + blocks, jnp.float32),
            dma((tp,)), dma((tp,)), dma((tp,)),
            dma((sp,)), dma((sp,)), *[dma((tp, split))] * 8, dma((2, tp, split)), dma((sp, tp, split)),
        ],
        compiler_params=pltpu.CompilerParams(collective_id=0, has_side_effects=True, vmem_limit_bytes=24 * 2 ** 20),
        name="tail",
    )(pay, x_in, gain[None, :], *(pltpu.with_memory_space_constraint(w, pltpu.HBM) for w in (w_out.reshape(width, d), w_up, w_down)))


def attend_kernel(lens_hbm, x_hbm, gain_hbm, w_hbm, k_hbm, v_hbm, pay_ref, kn_hbm, vn_hbm,
                  lens_ref, x_ref, gain_ref, wbuf, wide, normed, qkv, kbuf, vbuf, rep_k, rep_v, p_t,
                  small_in, w_in, k_in, v_in, k_out, v_out, *, heads, all_heads, sp, chunks, ahead):
    batch, pairs, hd = kbuf.shape
    slots = pairs // heads
    per = batch // chunks
    base = lax.axis_index("sp") * slots

    def moves(src, dst, sem, c):
        part = pl.ds(c * per, per)
        return pltpu.make_async_copy(src.at[part], dst.at[part], sem.at[c])

    small = [pltpu.make_async_copy(src, dst, small_in.at[i])
             for i, (src, dst) in enumerate(((x_hbm, x_ref), (gain_hbm, gain_ref), (lens_hbm, lens_ref)))]
    for copy in small:
        copy.start()
    d = x_ref.shape[1]
    parts = 3 * heads
    depth = wide.shape[0] // parts
    pieces = d // depth
    loads = []
    for j in range(pieces):
        part = pl.ds(j * depth * parts, depth * parts)
        loads.append(pltpu.make_async_copy(w_hbm.at[part], wbuf.at[part], w_in.at[j]))
    loads += [moves(k_hbm, kbuf, k_in, c) for c in range(chunks)] + [moves(v_hbm, vbuf, v_in, c) for c in range(chunks)]
    for copy in loads[:ahead]:
        copy.start()

    def loaded(i):
        loads[i].wait()
        if i + ahead < len(loads):
            loads[i + ahead].start()

    for copy in small:
        copy.wait()
    normed[...] = layer_norm(x_ref[...].astype(jnp.float32), gain_ref[...]).astype(jnp.bfloat16)
    proj = None
    for j in range(pieces):
        loaded(j)
        wide[...] = wbuf[j * depth * parts:(j + 1) * depth * parts, :].astype(jnp.float32)
        w = jnp.concatenate([wide[pl.ds(i, depth, stride=parts), :].astype(jnp.bfloat16) for i in range(parts)], axis=1)
        part = jnp.dot(normed[:, j * depth:(j + 1) * depth], w, preferred_element_type=jnp.float32)
        proj = part if proj is None else proj + part
    for i in range(parts):
        qkv[i // heads, pl.ds(i % heads, batch, stride=heads), :] = (
            proj[:, i * hd:(i + 1) * hd].astype(jnp.bfloat16).astype(jnp.float32))

    low = lax.broadcasted_iota(jnp.int32, (1, 8, hd), 1) < heads
    for rep, i in ((rep_k, 1), (rep_v, 2)):
        new = qkv[i].reshape(batch // 2, 8, hd)
        turned = pltpu.roll(new, heads, 1)
        rep[:, 0] = jnp.where(low, new, turned)
        rep[:, 1] = jnp.where(low, turned, new)

    row_slot = lax.broadcasted_iota(jnp.int32, (16, hd), 0) // heads

    def put_rows(buf, rep, c):
        for b in range(c * per, (c + 1) * per):
            slot = lens_ref[b] - base

            @pl.when((slot >= 0) & (slot < slots))
            def _():
                span = pl.ds(pl.multiple_of(slot // 4 * 16, 16), 16)
                old = buf[b, span, :].astype(jnp.float32)
                new = jnp.concatenate([rep[b // 2, b % 2]] * 2, axis=0)
                buf[b, span, :] = jnp.where(row_slot == lax.rem(slot, 4), new, old).astype(buf.dtype)

    def store_v(c):
        loaded(pieces + chunks + c)
        put_rows(vbuf, rep_v, c)
        moves(vbuf, vn_hbm, v_out, c).start()

    q_t = qkv[0].T.astype(jnp.bfloat16)
    lane = lax.broadcasted_iota(jnp.int32, (1, 128), 1)
    lane_seq, lane_head = lane // heads, lax.rem(lane, heads)
    group = 128 // heads
    row = lax.broadcasted_iota(jnp.int32, (pairs, 128), 0)
    pos = base + row // heads
    same_head = lax.rem(row, heads) == lane_head
    slope = jnp.exp2((lax.axis_index("tp") * heads + lane_head + 1).astype(jnp.float32) * (-8.0 / all_heads))
    per_group = chunks // (batch // group)
    for g in range(batch // group):
        q_g = q_t[:, g * 128:(g + 1) * 128]
        scores = None
        for c in range(g * per_group, (g + 1) * per_group):
            loaded(pieces + c)
            put_rows(kbuf, rep_k, c)
            seqs = range(c * per, (c + 1) * per)
            keys = jnp.concatenate([kbuf[b] for b in seqs], axis=1)
            query = jnp.concatenate([jnp.where(lane_seq == b - g * group, q_g, 0) for b in seqs], axis=0)
            part = jnp.dot(keys, query, preferred_element_type=jnp.float32)
            scores = part if scores is None else scores + part
            moves(kbuf, kn_hbm, k_out, c).start()
            if c > 0:
                store_v(c - 1)
        length = jnp.zeros((1, 128), jnp.int32)
        for i in range(group):
            length = jnp.where(lane_seq == i, lens_ref[g * group + i], length)
        scores = scores * hd ** -0.5 - slope * (length - pos).astype(jnp.float32)
        valid = same_head & (pos <= length)
        scores = jnp.where(valid, scores, -1e30)
        top = jnp.max(scores, axis=0, keepdims=True)
        p = jnp.where(valid, jnp.exp(scores - top), 0.0)
        total = jnp.sum(p, axis=0, keepdims=True)
        stats = jnp.concatenate([top, total, jnp.zeros((6, 128), jnp.float32)], axis=0)
        for s in range(g * sp // (batch // group), (g + 1) * sp // (batch // group)):
            pay_ref[s, batch // sp * heads:, :] = stats
        p_t[g * 128:(g + 1) * 128, :] = p.T.astype(jnp.bfloat16)

    quad = 16 // heads
    row_seq = lax.broadcasted_iota(jnp.int32, (16, hd), 0) // heads
    for c in range(chunks):
        if c == 0:
            store_v(chunks - 1)
        for b in range(c * per, (c + 1) * per, quad):
            values = jnp.concatenate([vbuf[b + i] for i in range(quad)], axis=1)
            out = jnp.dot(p_t[b * heads:b * heads + 16, :], values, preferred_element_type=jnp.float32)
            out = sum(jnp.where(row_seq == i, out[:, i * hd:(i + 1) * hd], 0.0) for i in range(quad))
            owner = b * sp // batch
            at = (b - owner * (batch // sp)) * heads
            pay_ref[owner, at:at + 16, :] = out
    for c in range(chunks):
        moves(kbuf, kn_hbm, k_out, c).wait()
        moves(vbuf, vn_hbm, v_out, c).wait()


def attend(tp, sp, lens, x_in, gain, w_qkv, k_cache, v_cache):
    batch, slots, heads, hd = k_cache.shape
    d = x_in.shape[1]
    chunks, pieces, ahead = 4, 4, 6
    flat = (batch, slots * heads, hd)
    vmem = pl.BlockSpec(memory_space=pltpu.VMEM)
    hbm = pl.BlockSpec(memory_space=pltpu.HBM)
    dma = pltpu.SemaphoreType.DMA
    operands = (lens, x_in, gain[None, :], w_qkv.reshape(d * 3 * heads, hd), k_cache.reshape(flat), v_cache.reshape(flat))
    pay, k_next, v_next = pl.pallas_call(
        functools.partial(attend_kernel, heads=heads, all_heads=heads * tp, sp=sp, chunks=chunks, ahead=ahead),
        out_shape=(jax.ShapeDtypeStruct((sp, batch // sp * heads + 8, hd), jnp.float32),
                   jax.ShapeDtypeStruct(flat, k_cache.dtype), jax.ShapeDtypeStruct(flat, v_cache.dtype)),
        in_specs=[hbm] * len(operands),
        out_specs=(vmem, hbm, hbm),
        scratch_shapes=[
            pltpu.SMEM(lens.shape, lens.dtype), pltpu.VMEM(x_in.shape, x_in.dtype), pltpu.VMEM((1, d), gain.dtype),
            pltpu.VMEM((d * 3 * heads, hd), jnp.bfloat16), pltpu.VMEM((d // pieces * 3 * heads, hd), jnp.float32),
            pltpu.VMEM((batch, d), jnp.bfloat16), pltpu.VMEM((3, batch * heads, hd), jnp.float32),
            pltpu.VMEM(flat, k_cache.dtype), pltpu.VMEM(flat, v_cache.dtype),
            pltpu.VMEM((batch // 2, 2, 8, hd), jnp.float32), pltpu.VMEM((batch // 2, 2, 8, hd), jnp.float32),
            pltpu.VMEM((batch * heads, slots * heads), jnp.bfloat16),
            dma((3,)), dma((pieces,)), dma((chunks,)), dma((chunks,)), dma((chunks,)), dma((chunks,)),
        ],
        compiler_params=pltpu.CompilerParams(vmem_limit_bytes=36 * 2 ** 20),
        name="attend",
    )(*(pltpu.with_memory_space_constraint(a, pltpu.HBM) for a in operands))
    return pay, k_next.reshape(k_cache.shape), v_next.reshape(v_cache.shape)


def solution(mesh):
    tp_size = mesh.shape["tp"]
    sp_size = mesh.shape["sp"]

    def local_layer(x_in, seq_lens, k_cache, v_cache, ln1_gain, w_qkv, w_out, ln2_gain, w_up, w_down):
        local_heads = k_cache.shape[2]
        head_dim = k_cache.shape[3]
        pay, k_next, v_next = attend(tp_size, sp_size, seq_lens, x_in, ln1_gain, w_qkv, k_cache, v_cache)
        x_out = tail(tp_size, sp_size, local_heads, head_dim, pay, x_in, ln2_gain, w_out, w_up, w_down)
        return x_out, k_next, v_next

    cache_spec = P("dp", "sp", "tp", None)
    in_specs = (P("dp", None), P("dp"), cache_spec, cache_spec, P(None), P(None, None, "tp", None), P("tp", None, None), P(None), P(None, "tp"), P("tp", None))
    out_specs = (P("dp", None), cache_spec, cache_spec)
    return jax.shard_map(local_layer, mesh=mesh, in_specs=in_specs, out_specs=out_specs, check_vma=False)
```

```python
import functools

import jax
import jax.numpy as jnp
from jax import lax
from jax.experimental import pallas as pl
from jax.experimental.pallas import tpu as pltpu
from jax.sharding import PartitionSpec as P

LN_EPS = 1e-5
MESH = pl.DeviceIdType.MESH


def layer_norm(x_f32, gain):
    mean = jnp.mean(x_f32, axis=-1, keepdims=True)
    centred = x_f32 - mean
    variance = jnp.mean(centred * centred, axis=-1, keepdims=True)
    return centred * lax.rsqrt(variance + LN_EPS) * gain


def gelu(x):
    return 0.5 * x * (1.0 + lax.erf(x * (0.5 ** 0.5)))


def tail_kernel(tp, sp, heads, hd, pay_ref, x_ref, gain_ref, wo_hbm, wu_hbm, wd_hbm, out_ref,
                wo, wu, wd, got_pay, att, part, got_part, r_all, h_mid, hidden, down, got_down, x_all,
                wo_sem, wu_sem, wd_sem, s1, r1, s2, r2, s3, r3, s4, r4, s5z, s5y, s5c, r5):
    my_tp = lax.axis_index("tp")
    my_sp = lax.axis_index("sp")
    rows = x_ref.shape[0] // sp
    cols = x_ref.shape[1] // tp

    barrier = pltpu.get_barrier_semaphore()
    for off in range(1, sp):
        pl.semaphore_signal(barrier, inc=1, device_id={"sp": lax.rem(my_sp + off, sp)}, device_id_type=MESH)
    for off in range(1, tp):
        pl.semaphore_signal(barrier, inc=1, device_id={"tp": lax.rem(my_tp + off, tp)}, device_id_type=MESH)

    loads = {}
    for name, src, dst, sem in (("o", wo_hbm, wo, wo_sem), ("u", wu_hbm, wu, wu_sem), ("d", wd_hbm, wd, wd_sem)):
        for j in range(tp):
            copy = pltpu.make_async_copy(src.at[:, pl.ds(j * cols, cols)], dst.at[j], sem.at[j])
            copy.start()
            loads[name, j] = copy

    pl.semaphore_wait(barrier, sp + tp - 2)

    side = lax.rem(my_sp + 2, sp)
    twin = my_sp + 1 - 2 * lax.rem(my_sp, 2)
    side_twin = lax.rem(twin + 2, sp)
    sends = []
    for off in range(1, sp):
        peer = lax.rem(my_sp + off, sp)
        copy = pltpu.make_async_remote_copy(
            pay_ref.at[peer], got_pay.at[my_sp],
            s1.at[off], r1.at[my_sp], device_id={"sp": peer}, device_id_type=MESH)
        copy.start()
        sends.append(copy)

    def arrived(dst, sem):
        pltpu.make_async_copy(dst, dst, sem).wait()

    pairs = rows * heads
    blocks = [pay_ref[my_sp]]
    for off in range(1, sp):
        peer = lax.rem(my_sp + off, sp)
        arrived(got_pay.at[peer], r1.at[peer])
        blocks.append(got_pay[peer])
    top = functools.reduce(jnp.maximum, [b[pairs:pairs + 1] for b in blocks])
    scale = [jnp.exp(b[pairs:pairs + 1] - top) for b in blocks]
    den = sum(c * b[pairs + 1:pairs + 2] for c, b in zip(scale, blocks))
    coef = jnp.concatenate(scale + [den] * (8 - sp), axis=0).T
    coef = jnp.where(lax.rem(my_sp, 2) == 0, coef[:pairs], coef[pairs:])
    att[...] = sum(coef[:, i:i + 1] * b[:pairs] for i, b in enumerate(blocks)) / coef[:, sp:sp + 1]
    attended = jnp.concatenate([att[pl.ds(h, rows, stride=heads), :] for h in range(heads)], axis=1).astype(jnp.bfloat16)

    high = my_tp // 2
    near = (my_tp + 1 - 2 * lax.rem(my_tp, 2), 2 - high, 3 - 3 * high)
    far = near[::-1]
    split = part.shape[1]
    piece = cols // split

    def send(src, dst, send_sem, recv_sem, to):
        copy = pltpu.make_async_remote_copy(src, dst, send_sem, recv_sem, device_id=to, device_id_type=MESH)
        copy.start()
        sends.append(copy)

    def reduce_scatter(lhs, weights, buf, got, send_sem, recv_sem):
        for i in range(split):
            for peer in far:
                buf[peer, i] = jnp.dot(lhs, weights[peer, :, i * piece:(i + 1) * piece], preferred_element_type=jnp.float32)
                send(buf.at[peer, i], got.at[my_tp, i], send_sem.at[peer, i], recv_sem.at[my_tp, i], {"tp": peer})
        own = [jnp.dot(lhs, weights[my_tp, :, i * piece:(i + 1) * piece], preferred_element_type=jnp.float32)
               for i in range(split)]

        def total(i):
            out = own[i]
            for peer in near:
                arrived(got.at[peer, i], recv_sem.at[peer, i])
                out += got[peer, i]
            return out
        return total

    for j in range(tp):
        loads["o", j].wait()
    total = reduce_scatter(attended, wo, part, got_part, s2, r2)
    row0 = pl.multiple_of(my_sp * rows, rows)
    for i in range(split):
        col0 = pl.multiple_of(my_tp * cols + i * piece, piece)
        r_all[my_tp, i] = total(i) + x_ref[pl.ds(row0, rows), pl.ds(col0, piece)].astype(jnp.float32)
        for peer in far:
            send(r_all.at[my_tp, i], r_all.at[my_tp, i], s3.at[peer, i], r3.at[my_tp, i], {"tp": peer})
    for i in range(split):
        for peer in near:
            arrived(r_all.at[peer, i], r3.at[peer, i])

    r = jnp.concatenate([r_all[j, i] for j in range(tp) for i in range(split)], axis=1)
    h_mid[...] = layer_norm(r, gain_ref[...]).astype(jnp.bfloat16)

    for j in range(tp):
        loads["u", j].wait()
        up = jnp.dot(h_mid[...], wu[j], preferred_element_type=jnp.float32)
        hidden[:, j * wu.shape[2]:(j + 1) * wu.shape[2]] = gelu(up).astype(jnp.bfloat16)

    for j in range(tp):
        loads["d", j].wait()
    total = reduce_scatter(hidden[...], wd, down, got_down, s4, r4)


    def pass_on(s, t, i, send_sem, to):
        send(x_all.at[s, t, i], x_all.at[s, t, i], send_sem, r5.at[s, t, i], to)

    for i in range(split):
        x_all[my_sp, my_tp, i] = (r_all[my_tp, i] + total(i)).astype(jnp.bfloat16).astype(jnp.float32)
        for peer in far:
            pass_on(my_sp, my_tp, i, s5y.at[peer, i], {"tp": peer, "sp": side})
            pass_on(my_sp, my_tp, i, s5z.at[peer, i], {"tp": peer})
        pass_on(my_sp, my_tp, i, s5y.at[my_tp, i], {"sp": side})
        pass_on(my_sp, my_tp, i, s5c.at[0, my_tp, i], {"sp": twin})
    for i in range(split):
        arrived(x_all.at[side, my_tp, i], r5.at[side, my_tp, i])
        pass_on(side, my_tp, i, s5c.at[1, my_tp, i], {"sp": twin})
        for peer in near:
            for n, who in enumerate((my_sp, side)):
                arrived(x_all.at[who, peer, i], r5.at[who, peer, i])
                pass_on(who, peer, i, s5c.at[n, peer, i], {"sp": twin})
    for who in (twin, side_twin):
        for i in range(split):
            for peer in (my_tp,) + near:
                arrived(x_all.at[who, peer, i], r5.at[who, peer, i])
    for s in range(sp):
        for t in range(tp):
            for i in range(split):
                at = t * cols + i * piece
                out_ref[s * rows:(s + 1) * rows, at:at + piece] = x_all[s, t, i].astype(jnp.bfloat16)
    for copy in sends:
        copy.wait_send()


def tail(tp, sp, heads, hd, pay, x_in, gain, w_out, w_up, w_down):
    batch, d = x_in.shape
    rows, cols = batch // sp, d // tp
    split = 1
    blocks = (tp, split, rows, cols // split)
    ff = w_up.shape[1]
    width = heads * hd
    vmem = pl.BlockSpec(memory_space=pltpu.VMEM)
    hbm = pl.BlockSpec(memory_space=pltpu.HBM)
    dma = pltpu.SemaphoreType.DMA
    return pl.pallas_call(
        functools.partial(tail_kernel, tp, sp, heads, hd),
        out_shape=jax.ShapeDtypeStruct((batch, d), jnp.bfloat16),
        in_specs=[vmem, vmem, vmem, hbm, hbm, hbm],
        out_specs=vmem,
        scratch_shapes=[
            pltpu.VMEM((tp, width, cols), jnp.bfloat16),
            pltpu.VMEM((tp, d, ff // tp), jnp.bfloat16),
            pltpu.VMEM((tp, ff, cols), jnp.bfloat16),
            pltpu.VMEM(pay.shape, jnp.float32),
            pltpu.VMEM((rows * heads, hd), jnp.float32),
            pltpu.VMEM(blocks, jnp.float32), pltpu.VMEM(blocks, jnp.float32), pltpu.VMEM(blocks, jnp.float32),
            pltpu.VMEM((rows, d), jnp.bfloat16),
            pltpu.VMEM((rows, ff), jnp.bfloat16),
            pltpu.VMEM(blocks, jnp.float32), pltpu.VMEM(blocks, jnp.float32),
            pltpu.VMEM((sp,) + blocks, jnp.float32),
            dma((tp,)), dma((tp,)), dma((tp,)),
            dma((sp,)), dma((sp,)), *[dma((tp, split))] * 8, dma((2, tp, split)), dma((sp, tp, split)),
        ],
        compiler_params=pltpu.CompilerParams(collective_id=0, has_side_effects=True, vmem_limit_bytes=24 * 2 ** 20),
        name="tail",
    )(pay, x_in, gain[None, :], *(pltpu.with_memory_space_constraint(w, pltpu.HBM) for w in (w_out.reshape(width, d), w_up, w_down)))


def attend_kernel(lens_hbm, x_hbm, gain_hbm, w_hbm, k_hbm, v_hbm, pay_ref, kn_hbm, vn_hbm,
                  lens_ref, x_ref, gain_ref, wbuf, wide, normed, qkv, kbuf, vbuf, rep_k, rep_v, p_t,
                  small_in, w_in, k_in, v_in, k_out, v_out, *, heads, all_heads, sp, chunks, ahead):
    batch, pairs, hd = kbuf.shape
    slots = pairs // heads
    per = batch // chunks
    base = lax.axis_index("sp") * slots

    def moves(src, dst, sem, c):
        part = pl.ds(c * per, per)
        return pltpu.make_async_copy(src.at[part], dst.at[part], sem.at[c])

    small = [pltpu.make_async_copy(src, dst, small_in.at[i])
             for i, (src, dst) in enumerate(((x_hbm, x_ref), (gain_hbm, gain_ref), (lens_hbm, lens_ref)))]
    for copy in small:
        copy.start()
    d = x_ref.shape[1]
    parts = 3 * heads
    depth = wide.shape[0] // parts
    pieces = d // depth
    loads = []
    for j in range(pieces):
        part = pl.ds(j * depth * parts, depth * parts)
        loads.append(pltpu.make_async_copy(w_hbm.at[part], wbuf.at[part], w_in.at[j]))
    loads += [moves(k_hbm, kbuf, k_in, c) for c in range(chunks)] + [moves(v_hbm, vbuf, v_in, c) for c in range(chunks)]
    for copy in loads[:ahead]:
        copy.start()

    def loaded(i):
        loads[i].wait()
        if i + ahead < len(loads):
            loads[i + ahead].start()

    for copy in small:
        copy.wait()
    normed[...] = layer_norm(x_ref[...].astype(jnp.float32), gain_ref[...]).astype(jnp.bfloat16)
    proj = None
    for j in range(pieces):
        loaded(j)
        wide[...] = wbuf[j * depth * parts:(j + 1) * depth * parts, :].astype(jnp.float32)
        w = jnp.concatenate([wide[pl.ds(i, depth, stride=parts), :].astype(jnp.bfloat16) for i in range(parts)], axis=1)
        part = jnp.dot(normed[:, j * depth:(j + 1) * depth], w, preferred_element_type=jnp.float32)
        proj = part if proj is None else proj + part
    for i in range(parts):
        qkv[i // heads, pl.ds(i % heads, batch, stride=heads), :] = (
            proj[:, i * hd:(i + 1) * hd].astype(jnp.bfloat16).astype(jnp.float32))

    low = lax.broadcasted_iota(jnp.int32, (1, 8, hd), 1) < heads
    for rep, i in ((rep_k, 1), (rep_v, 2)):
        new = qkv[i].reshape(batch // 2, 8, hd)
        turned = pltpu.roll(new, heads, 1)
        rep[:, 0] = jnp.where(low, new, turned)
        rep[:, 1] = jnp.where(low, turned, new)

    row_slot = lax.broadcasted_iota(jnp.int32, (16, hd), 0) // heads

    def put_rows(buf, rep, c):
        for b in range(c * per, (c + 1) * per):
            slot = lens_ref[b] - base

            @pl.when((slot >= 0) & (slot < slots))
            def _():
                span = pl.ds(pl.multiple_of(slot // 4 * 16, 16), 16)
                old = buf[b, span, :].astype(jnp.float32)
                new = jnp.concatenate([rep[b // 2, b % 2]] * 2, axis=0)
                buf[b, span, :] = jnp.where(row_slot == lax.rem(slot, 4), new, old).astype(buf.dtype)

    def store_v(c):
        loaded(pieces + chunks + c)
        put_rows(vbuf, rep_v, c)
        moves(vbuf, vn_hbm, v_out, c).start()

    q_t = qkv[0].T.astype(jnp.bfloat16)
    lane = lax.broadcasted_iota(jnp.int32, (1, 128), 1)
    lane_seq, lane_head = lane // heads, lax.rem(lane, heads)
    group = 128 // heads
    row = lax.broadcasted_iota(jnp.int32, (pairs, 128), 0)
    pos = base + row // heads
    same_head = lax.rem(row, heads) == lane_head
    slope = jnp.exp2((lax.axis_index("tp") * heads + lane_head + 1).astype(jnp.float32) * (-8.0 / all_heads))
    per_group = chunks // (batch // group)
    for g in range(batch // group):
        q_g = q_t[:, g * 128:(g + 1) * 128]
        scores = None
        for c in range(g * per_group, (g + 1) * per_group):
            loaded(pieces + c)
            put_rows(kbuf, rep_k, c)
            seqs = range(c * per, (c + 1) * per)
            keys = jnp.concatenate([kbuf[b] for b in seqs], axis=1)
            query = jnp.concatenate([jnp.where(lane_seq == b - g * group, q_g, 0) for b in seqs], axis=0)
            part = jnp.dot(keys, query, preferred_element_type=jnp.float32)
            scores = part if scores is None else scores + part
            moves(kbuf, kn_hbm, k_out, c).start()
            if c > 0:
                store_v(c - 1)
        length = jnp.zeros((1, 128), jnp.int32)
        for i in range(group):
            length = jnp.where(lane_seq == i, lens_ref[g * group + i], length)
        scores = scores * hd ** -0.5 - slope * (length - pos).astype(jnp.float32)
        valid = same_head & (pos <= length)
        scores = jnp.where(valid, scores, -1e30)
        top = jnp.max(scores, axis=0, keepdims=True)
        p = jnp.where(valid, jnp.exp(scores - top), 0.0)
        total = jnp.sum(p, axis=0, keepdims=True)
        stats = jnp.concatenate([top, total, jnp.zeros((6, 128), jnp.float32)], axis=0)
        for s in range(g * sp // (batch // group), (g + 1) * sp // (batch // group)):
            pay_ref[s, batch // sp * heads:, :] = stats
        p_t[g * 128:(g + 1) * 128, :] = p.T.astype(jnp.bfloat16)

    quad = 16 // heads
    row_seq = lax.broadcasted_iota(jnp.int32, (16, hd), 0) // heads
    for c in range(chunks):
        if c == 0:
            store_v(chunks - 1)
        for b in range(c * per, (c + 1) * per, quad):
            values = jnp.concatenate([vbuf[b + i] for i in range(quad)], axis=1)
            out = jnp.dot(p_t[b * heads:b * heads + 16, :], values, preferred_element_type=jnp.float32)
            out = sum(jnp.where(row_seq == i, out[:, i * hd:(i + 1) * hd], 0.0) for i in range(quad))
            owner = b * sp // batch
            at = (b - owner * (batch // sp)) * heads
            pay_ref[owner, at:at + 16, :] = out
    for c in range(chunks):
        moves(kbuf, kn_hbm, k_out, c).wait()
        moves(vbuf, vn_hbm, v_out, c).wait()


def attend(tp, sp, lens, x_in, gain, w_qkv, k_cache, v_cache):
    batch, slots, heads, hd = k_cache.shape
    d = x_in.shape[1]
    chunks, pieces, ahead = 4, 4, 6
    flat = (batch, slots * heads, hd)
    vmem = pl.BlockSpec(memory_space=pltpu.VMEM)
    hbm = pl.BlockSpec(memory_space=pltpu.HBM)
    dma = pltpu.SemaphoreType.DMA
    operands = (lens, x_in, gain[None, :], w_qkv.reshape(d * 3 * heads, hd), k_cache.reshape(flat), v_cache.reshape(flat))
    pay, k_next, v_next = pl.pallas_call(
        functools.partial(attend_kernel, heads=heads, all_heads=heads * tp, sp=sp, chunks=chunks, ahead=ahead),
        out_shape=(jax.ShapeDtypeStruct((sp, batch // sp * heads + 8, hd), jnp.float32),
                   jax.ShapeDtypeStruct(flat, k_cache.dtype), jax.ShapeDtypeStruct(flat, v_cache.dtype)),
        in_specs=[hbm] * len(operands),
        out_specs=(vmem, hbm, hbm),
        scratch_shapes=[
            pltpu.SMEM(lens.shape, lens.dtype), pltpu.VMEM(x_in.shape, x_in.dtype), pltpu.VMEM((1, d), gain.dtype),
            pltpu.VMEM((d * 3 * heads, hd), jnp.bfloat16), pltpu.VMEM((d // pieces * 3 * heads, hd), jnp.float32),
            pltpu.VMEM((batch, d), jnp.bfloat16), pltpu.VMEM((3, batch * heads, hd), jnp.float32),
            pltpu.VMEM(flat, k_cache.dtype), pltpu.VMEM(flat, v_cache.dtype),
            pltpu.VMEM((batch // 2, 2, 8, hd), jnp.float32), pltpu.VMEM((batch // 2, 2, 8, hd), jnp.float32),
            pltpu.VMEM((batch * heads, slots * heads), jnp.bfloat16),
            dma((3,)), dma((pieces,)), dma((chunks,)), dma((chunks,)), dma((chunks,)), dma((chunks,)),
        ],
        compiler_params=pltpu.CompilerParams(vmem_limit_bytes=36 * 2 ** 20),
        name="attend",
    )(*(pltpu.with_memory_space_constraint(a, pltpu.HBM) for a in operands))
    return pay, k_next.reshape(k_cache.shape), v_next.reshape(v_cache.shape)


def solution(mesh):
    tp_size = mesh.shape["tp"]
    sp_size = mesh.shape["sp"]

    def local_layer(x_in, seq_lens, k_cache, v_cache, ln1_gain, w_qkv, w_out, ln2_gain, w_up, w_down):
        local_heads = k_cache.shape[2]
        head_dim = k_cache.shape[3]
        pay, k_next, v_next = attend(tp_size, sp_size, seq_lens, x_in, ln1_gain, w_qkv, k_cache, v_cache)
        x_out = tail(tp_size, sp_size, local_heads, head_dim, pay, x_in, ln2_gain, w_out, w_up, w_down)
        return x_out, k_next, v_next

    cache_spec = P("dp", "sp", "tp", None)
    in_specs = (P("dp", None), P("dp"), cache_spec, cache_spec, P(None), P(None, None, "tp", None), P("tp", None, None), P(None), P(None, "tp"), P("tp", None))
    out_specs = (P("dp", None), cache_spec, cache_spec)
    return jax.shard_map(local_layer, mesh=mesh, in_specs=in_specs, out_specs=out_specs, check_vma=False)
```
